512 devices in a mesh: pair: 64 (over z, y), split: 8 (over x, core).
Axes of the slice: x: 4, y: 8, z: 8, core: 2. Of those that a mesh axis runs over, the one named last changes fastest.
Arguments:
- descriptors: bfloat16 [64, 1024, 256], P('pair', 'split'), as said below
- points: bfloat16 [64, 3, 1024], P('pair', None, 'split'), may hold values from -6 to 6
- normals: bfloat16 [64, 3, 1024], P('pair', None, 'split'), may hold values from -6 to 6
- pair_list: int32 [1536, 2], replicated, may hold values from 0 to 63, as said below
- intersection: int32 [1536], P('pair'), may hold values from 256 to 1024
- pose_index: int32 [64], replicated, may hold values from 0 to 63, each once
Outputs:
- pair_cross: float32 [1536, 6, 6], P('pair')
- pose_hessian: float32 [64, 6, 6], P('pair')
- pose_gradient: float32 [64, 6], P('pair')
The draws below stay inside these ranges and needn't reach their ends.
Inputs may be any that keep to these rules, and one draw needn't show every extreme that they name: `descriptors`: values stay within -24 to 24. `pair_list`: task k's source scan is scan k // 24. The owner of a scan s is s; a task's target has another owner than its source. Among the 24 tasks of one aligned block (tasks k // 24 alike), no owner holds the targets of more than 1 of them, and some owner holds exactly 1.
All inputs are finite; a program needn't handle non-finite values.
Results may differ from the reference program's by a relative error of at most 0.0003.
Values may be sent and summed in bfloat16 or wider, within the bound.
No kernel may reach another device: no remote copies, remote signals or barrier semaphores. Data moves between devices by JAX's collectives and lax.ppermute only.
A program may use at most 64 MiB of HBM per device.

```python
import jax
import jax.numpy as jnp
from jax import lax

C = 256
S = 1024
SCAN_DEV = 1
PAIR_DEV = 24
CAP = 1
SCANS = 64
PAIRS = 1536
N_PAIR = 64


def draw_descriptors(key, part):
    key_base = jax.random.fold_in(key, 0)
    values = jnp.clip(jax.random.normal(key_base, (SCANS, S, C), jnp.float32), -4.0, 4.0)
    return values.astype(jnp.bfloat16)


def draw_pair_list(key, part):
    key_source, key_order, key_local = jax.random.split(key, 3)
    owners = jnp.arange(N_PAIR, dtype=jnp.int32)
    source_local = jax.random.randint(key_source, (N_PAIR, PAIR_DEV), 0, SCAN_DEV, jnp.int32)
    sources = owners[:, None] * SCAN_DEV + source_local
    order_keys = jax.random.split(key_order, N_PAIR * CAP)
    offsets = jax.vmap(lambda single: jax.random.permutation(single, N_PAIR - 1))(order_keys)
    offsets = offsets.reshape(N_PAIR, CAP * (N_PAIR - 1))[:, :PAIR_DEV].astype(jnp.int32)
    holder = (owners[:, None] + 1 + offsets) % N_PAIR
    targets = holder * SCAN_DEV + jax.random.randint(key_local, (N_PAIR, PAIR_DEV), 0, SCAN_DEV, jnp.int32)
    return jnp.stack([sources, targets], axis=-1).reshape(PAIRS, 2).astype(jnp.int32)


def with_ends(values, key, least, largest):
    index_at = [jax.random.randint(jax.random.fold_in(key, axis), (), 0, length) for axis, length in enumerate(values.shape)]
    widest = values.shape.index(max(values.shape))
    neighbour = index_at[:widest] + [(index_at[widest] + 1) % values.shape[widest]] + index_at[widest + 1:]
    return values.at[tuple(index_at)].set(least).at[tuple(neighbour)].set(largest)


def block_levels(own_key, extent, pieces, least, top_value):
    def one(position, shards_of):
        draws = jax.random.uniform(jax.random.fold_in(jax.random.fold_in(own_key, 6), position), (shards_of,), jnp.float32, least / len(pieces), top_value / len(pieces))
        return jnp.repeat(jnp.exp(draws), extent[position] // shards_of).reshape((-1,) + (1,) * (len(extent) - position - 1))

    gain = one(*pieces[0])
    for cut in pieces[1:]:
        gain = gain * one(*cut)
    return gain


def noise(key, shape, spread, most, shards=(), kind=jnp.bfloat16):
    values = jax.random.normal(key, shape, jnp.float32) * spread
    if len(shards) > 0:
        values = block_levels(key, shape, shards, -0.22, 0.18) * values
    return jnp.clip(values, min=-most, max=most).astype(kind)


def setup_inputs(seed: int = 0) -> dict:
    key_list = jax.random.split(jax.random.key(seed), 7)
    return {
        "descriptors": draw_descriptors(jax.random.fold_in(key_list[6], 71), 0),
        "points": noise(key_list[1], (SCANS, 3, S), 1.0, 6.0, ((0, 64), (2, 8))),
        "normals": noise(key_list[2], (SCANS, 3, S), 1.0, 6.0, ((0, 64), (2, 8))),
        "pair_list": draw_pair_list(jax.random.fold_in(key_list[6], 71), 0),
        "intersection": with_ends(jax.random.randint(key_list[4], (PAIRS,), S // 4, S + 1), jax.random.fold_in(key_list[4], 1), S // 4, S).astype(jnp.int32),
        "pose_index": jax.random.permutation(key_list[5], SCANS).astype(jnp.int32),
    }


def cross_first(left_vec, right_vec):
    return jnp.stack([left_vec[1] * right_vec[2] - left_vec[2] * right_vec[1],
                      left_vec[2] * right_vec[0] - left_vec[0] * right_vec[2],
                      left_vec[0] * right_vec[1] - left_vec[1] * right_vec[0]], axis=0)


def reference(descriptors, points, normals, pair_list, intersection, pose_index):
    score_scale = descriptors.shape[2] ** -0.5
    row_ids = jnp.arange(S, dtype=jnp.int32)
    highest = lax.Precision.HIGHEST
    points_value = points.astype(jnp.float32)
    normals_value = normals.astype(jnp.float32)

    def one_task(task_row):
        source_id = task_row[0]
        target_id = task_row[1]
        live_rows = task_row[2]
        scores = jnp.dot(descriptors[source_id], descriptors[target_id].T, preferred_element_type=jnp.float32) * score_scale
        weights = jax.nn.softmax(scores, axis=1)
        geometry = jnp.concatenate([points_value[target_id], normals_value[target_id]], axis=0)
        softened = jnp.dot(geometry, weights.T, precision=highest)
        matched = softened[:3]
        normal = softened[3:]
        source = points_value[source_id]
        jacobian = jnp.concatenate([cross_first(source, normal), normal, -cross_first(matched, normal), -normal], axis=0)
        residual = jnp.sum(normal * (source - matched), axis=0)
        weight = (row_ids < live_rows).astype(jnp.float32)
        hessian = jnp.dot(jacobian * weight, jacobian.T, precision=highest) / S
        gradient = jnp.dot(jacobian * weight, residual, precision=highest) / S
        return hessian, gradient

    task_table = jnp.concatenate([pair_list, intersection[:, None]], axis=1).astype(jnp.int32)
    hessian, gradient = lax.map(one_task, task_table)
    pair_cross = hessian[:, :6, 6:]
    source_pose = pose_index[pair_list[:, 0]]
    target_pose = pose_index[pair_list[:, 1]]
    source_part = jnp.concatenate([hessian[:, :6, :6].reshape(-1, 36), gradient[:, :6]], axis=1)
    target_part = jnp.concatenate([hessian[:, 6:, 6:].reshape(-1, 36), gradient[:, 6:]], axis=1)
    pose_slots = jnp.arange(SCANS, dtype=jnp.int32)[:, None]
    onehot_source = (pose_slots == source_pose[None, :]).astype(jnp.float32)
    onehot_target = (pose_slots == target_pose[None, :]).astype(jnp.float32)
    totals = (jnp.dot(onehot_source, source_part, precision=highest) + jnp.dot(onehot_target, target_part, precision=highest)) / PAIR_DEV
    return pair_cross, totals[:, :36].reshape(-1, 6, 6), totals[:, 36:]
```

```python
import math

import jax
import jax.numpy as jnp
from jax import lax
from jax.experimental import pallas as pl
from jax.experimental.pallas import tpu as pltpu
from jax.sharding import PartitionSpec as P

SIDE = 8
PAIRS_PER = 24
QUADS = SIDE // 2
SOURCES = 2 * SIDE
SLOTS = SOURCES * QUADS
ROWS = 128
WIDTH = 256
EXTRA = 8
PACKED = ROWS + EXTRA
LANES = 128
POSE = 42
HIGHEST = lax.Precision.HIGHEST

y_groups = [[z * SIDE + y for y in range(SIDE)] for z in range(SIDE)]
z_groups = [[(par + 2 * q) * SIDE + y for q in range(QUADS)] for par in range(2) for y in range(SIDE)]
x_groups = [[2 * x + core for x in range(4)] for core in range(2)]
z_swap = [(z * SIDE + y, (z ^ 1) * SIDE + y) for z in range(SIDE) for y in range(SIDE)]
core_swap = [(s, s ^ 1) for s in range(8)]


def to_each(block, axis, groups):
    copies = jnp.broadcast_to(block, (len(groups[0]), *block.shape))
    return lax.all_to_all(copies, axis, split_axis=0, concat_axis=0, tiled=True, axis_index_groups=groups)


def nt(left, right, precision=None):
    return lax.dot_general(
        left, right, (((1,), (1,)), ((), ())), precision=precision, preferred_element_type=jnp.float32
    )


def cross_rows(u, v):
    return [
        u[1] * v[2] - u[2] * v[1],
        u[2] * v[0] - u[0] * v[2],
        u[0] * v[1] - u[1] * v[0],
    ]


def attend_kernel(scale, cnt_ref, base_ref, dst_ref, a1_ref, a2_ref, b1_ref, b2_ref, out_ref, a_ref, g_ref, h_ref, list_ref):
    a_ref[0:SIDE] = a1_ref[...]
    a_ref[SIDE:SOURCES] = a2_ref[...]
    for q in range(QUADS):
        for c, ref in enumerate((b1_ref, b2_ref)):
            for x in range(4):
                at = (c * 4 + x) * LANES
                g_ref[q, :, at : at + LANES] = ref[x, q, ROWS:PACKED, 0:LANES]
    h_ref[...] = jnp.zeros_like(h_ref)

    def scan(f, n):
        live = cnt_ref[f] > 0

        @pl.when(live)
        def _():
            list_ref[n] = f

        return n + live.astype(jnp.int32)

    n = lax.fori_loop(0, SLOTS, scan, jnp.int32(0))
    list_ref[n] = jnp.int32(SLOTS)
    row_ids = lax.broadcasted_iota(jnp.int32, (1, LANES), 1) + base_ref[0]

    def one(f):
        at = jnp.minimum(f, SLOTS - 1)
        q = at // SOURCES
        ia = at % SOURCES
        keys = jnp.concatenate(
            [ref[x, q, 0:ROWS, :] for ref in (b1_ref, b2_ref) for x in range(4)], axis=0
        )
        scores = nt(keys, a_ref[ia, 0:ROWS, :])
        top = jnp.max(scores, axis=0, keepdims=True)
        weights = jnp.exp2((scores - top) * scale)
        high = weights.astype(jnp.bfloat16)
        low = (weights - high.astype(jnp.float32)).astype(jnp.bfloat16)
        geometry = g_ref[q]
        moment = jnp.dot(geometry, high, preferred_element_type=jnp.float32) + jnp.dot(
            geometry, low, preferred_element_type=jnp.float32
        )
        softened = moment / moment[6:7]
        m = [softened[d : d + 1] for d in range(3)]
        v = [softened[3 + d : 4 + d] for d in range(3)]
        own = a_ref[ia, ROWS:PACKED, 0:LANES].astype(jnp.float32)
        s = [own[d : d + 1] for d in range(3)]
        residual = v[0] * (s[0] - m[0]) + v[1] * (s[1] - m[1]) + v[2] * (s[2] - m[2])
        zero = jnp.zeros_like(residual)
        jacobian = jnp.concatenate(
            cross_rows(s, v) + v + [-t for t in cross_rows(m, v)] + [-t for t in v] + [residual] + [zero] * 3,
            axis=0,
        )
        seen = (row_ids < cnt_ref[f]).astype(jnp.float32)
        h_ref[f] = nt(jacobian * seen, jacobian, HIGHEST)

    def two(t, carry):
        first = list_ref[2 * t]
        second = list_ref[2 * t + 1]
        one(first)
        one(second)
        return carry

    list_ref[n + 1] = jnp.int32(SLOTS)
    lax.fori_loop(0, (n + 1) // 2, two, 0)

    col = lax.broadcasted_iota(jnp.int32, (16, LANES), 0)
    lane = lax.broadcasted_iota(jnp.int32, (16, LANES), 1)
    flat_source = jnp.zeros((SLOTS, LANES), jnp.float32)
    flat_target = jnp.zeros((SLOTS, LANES), jnp.float32)
    flat_cross = jnp.zeros((SLOTS, LANES), jnp.float32)
    for r in range(6):
        tail = (col == 12) & (lane == 36 + r)
        pick_low = (((col < 6) & (lane == 6 * r + col)) | tail).astype(jnp.float32)
        in_high = (col >= 6) & (col < 12) & (lane == 6 * r + col - 6)
        pick_high = (in_high | tail).astype(jnp.float32)
        upper = h_ref[0:SLOTS, r, :]
        lower = h_ref[0:SLOTS, 6 + r, :]
        flat_source += jnp.dot(upper, pick_low, precision=HIGHEST, preferred_element_type=jnp.float32)
        flat_cross += jnp.dot(upper, in_high.astype(jnp.float32), precision=HIGHEST, preferred_element_type=jnp.float32)
        flat_target += jnp.dot(lower, pick_high, precision=HIGHEST, preferred_element_type=jnp.float32)
    dest = lax.broadcasted_iota(jnp.int32, (SIDE * SIDE, SLOTS), 0)
    to_source = (dest == dst_ref[0:1, :]).astype(jnp.float32)
    to_target = (dest == dst_ref[1:2, :]).astype(jnp.float32)
    to_owner = (dest == dst_ref[2:3, :]).astype(jnp.float32)
    pose = jnp.dot(to_source, flat_source, precision=HIGHEST, preferred_element_type=jnp.float32)
    pose += jnp.dot(to_target, flat_target, precision=HIGHEST, preferred_element_type=jnp.float32)
    owned = []
    for q in range(QUADS):
        here = slice(q * SOURCES, (q + 1) * SOURCES)
        moved = pltpu.roll(flat_cross[here], POSE + 36 * (q % 2), 1)
        owned.append(
            jnp.dot(to_owner[:, 0:SOURCES], moved, precision=HIGHEST, preferred_element_type=jnp.float32)
        )
    out_ref[:, 0, :] = pose + owned[0] + owned[1]
    out_ref[:, 1, :] = owned[2] + owned[3]


def collect_kernel(group_ref, quad_ref, got_ref, out_ref, even_ref, odd_ref):
    even_ref[...] = jnp.zeros_like(even_ref)
    odd_ref[...] = jnp.zeros_like(odd_ref)
    for t in range(PAIRS_PER):
        q = quad_ref[t]
        row = got_ref[group_ref[t], q // 2, :].reshape(1, LANES)
        side = (q % 2).astype(jnp.float32)
        even_ref[t : t + 1, :] = row * (1.0 - side)
        odd_ref[t : t + 1, :] = row * side
    even = pltpu.roll(even_ref[...], LANES - POSE, 1)
    odd = pltpu.roll(odd_ref[...], LANES - POSE - 36, 1)
    pose = jnp.sum(got_ref[:, 0, :], axis=0, keepdims=True)
    row_id = lax.broadcasted_iota(jnp.int32, (32, LANES), 0)
    both = jnp.where(row_id == PAIRS_PER, pose, even + odd)
    for s in range(8):
        out_ref[s] = both


def finish_kernel(task_scale, pose_scale, got_ref, cross_ref, hessian_ref, gradient_ref):
    total = got_ref[0]
    for s in range(1, 8):
        total += got_ref[s]
    pose = total[PAIRS_PER : PAIRS_PER + 1, :] * pose_scale
    padded = jnp.concatenate([total, jnp.zeros((LANES - 32, LANES), jnp.float32)], axis=0) * task_scale
    turned = padded.T
    for r in range(6):
        cross_ref[r] = turned[6 * r : 6 * r + 6, 0:PAIRS_PER]
        hessian_ref[r] = pose[:, 6 * r : 6 * r + 6]
    gradient_ref[...] = pose[:, 36:42]


def looked_up(table, ids):
    at = jnp.arange(table.shape[0], dtype=jnp.int32)
    return jnp.sum(jnp.where(at[None, :] == ids[:, None], table[None, :], 0), axis=1)


def per_device(descriptors, points, normals, pair_list, intersection, pose_index):
    own = lax.axis_index("pair")
    z, y = own // SIDE, own % SIDE
    parity = z % 2
    other = z + 1 - 2 * parity

    count_high = (intersection // 16).astype(jnp.bfloat16)
    count_low = (intersection % 16).astype(jnp.bfloat16)
    left = jnp.concatenate(
        [points[0], normals[0], jnp.ones((1, ROWS), jnp.bfloat16), jnp.zeros((1, ROWS), jnp.bfloat16)], axis=0
    )
    counts = jnp.pad(jnp.stack([count_high, count_low]), ((6, 0), (0, LANES - PAIRS_PER)))
    packed = jnp.concatenate([descriptors[0], jnp.concatenate([left, counts], axis=1)], axis=0)

    targets_quad = to_each(packed, "pair", z_groups)
    sources_row = to_each(packed, "pair", y_groups)
    targets_mine = to_each(targets_quad, "split", x_groups)
    sources_next = lax.ppermute(sources_row, "pair", z_swap)
    targets_peer = lax.ppermute(targets_mine, "split", core_swap)

    all_targets = pair_list[:, 1].reshape(SIDE, SIDE, PAIRS_PER)
    task_targets = jnp.concatenate(
        [lax.dynamic_slice_in_dim(all_targets, z, 1, 0)[0], lax.dynamic_slice_in_dim(all_targets, other, 1, 0)[0]], axis=0
    )
    quads = jnp.arange(QUADS, dtype=jnp.int32)
    target_ids = (parity + 2 * quads) * SIDE + y
    is_task = task_targets[None, :, :] == target_ids[:, None, None]
    both = jnp.concatenate([sources_row[:, ROWS + 6 :, LANES:], sources_next[:, ROWS + 6 :, LANES:]], axis=0)
    both = both[:, :, :PAIRS_PER].astype(jnp.float32)
    seen_rows = (both[:, 0] * 16 + both[:, 1]).astype(jnp.int32)
    task_counts = jnp.sum(jnp.where(is_task, seen_rows[None], 0), axis=2).reshape(SLOTS)
    task_counts = jnp.pad(task_counts, (0, 64))

    slot = jnp.arange(SLOTS, dtype=jnp.int32)
    slot_source = slot % SOURCES
    source_ids = jnp.where(slot_source < SIDE, z * SIDE + slot_source, other * SIDE + slot_source - SIDE)
    slot_targets = (parity + 2 * (slot // SOURCES)) * SIDE + y
    destinations = jnp.stack(
        [looked_up(pose_index, source_ids), looked_up(pose_index, slot_targets), source_ids] + [slot] * 5
    )
    base = (lax.axis_index("split") * ROWS).reshape(1)

    smem = pl.BlockSpec(memory_space=pltpu.SMEM)
    vmem = pl.BlockSpec(memory_space=pltpu.VMEM)
    scale = WIDTH**-0.5 / math.log(2.0)
    send = pl.pallas_call(
        lambda *refs: attend_kernel(scale, *refs),
        out_shape=jax.ShapeDtypeStruct((SIDE * SIDE, 2, LANES), jnp.float32),
        in_specs=[smem, smem, vmem, vmem, vmem, vmem, vmem],
        out_specs=vmem,
        scratch_shapes=[
            pltpu.VMEM((SOURCES, PACKED, WIDTH), jnp.bfloat16),
            pltpu.VMEM((QUADS, EXTRA, 8 * LANES), jnp.bfloat16),
            pltpu.VMEM((SLOTS + 1, 16, 16), jnp.float32),
            pltpu.SMEM((SLOTS + 8,), jnp.int32),
        ],
        compiler_params=pltpu.CompilerParams(vmem_limit_bytes=48 * 1024 * 1024),
        name="attend",
    )(task_counts, base, destinations, sources_row, sources_next, targets_mine, targets_peer)
    got = lax.all_to_all(send, "pair", split_axis=0, concat_axis=0, tiled=True)

    my_targets = lax.dynamic_slice_in_dim(pair_list[:, 1], own * PAIRS_PER, PAIRS_PER, 0)
    target_z, target_y = my_targets // SIDE, my_targets % SIDE
    group = jnp.where(target_z % 2 == parity, z, other) * SIDE + target_y
    share = pl.pallas_call(
        collect_kernel,
        out_shape=jax.ShapeDtypeStruct((8, 32, LANES), jnp.float32),
        in_specs=[smem, smem, vmem],
        out_specs=vmem,
        scratch_shapes=[pltpu.VMEM((32, LANES), jnp.float32), pltpu.VMEM((32, LANES), jnp.float32)],
        name="collect",
    )(group, target_z // 2, got)
    shares = lax.all_to_all(share, "split", split_axis=0, concat_axis=0, tiled=True)

    task_scale = 1.0 / (ROWS * 8)
    cross, hessian, gradient = pl.pallas_call(
        lambda *refs: finish_kernel(task_scale, task_scale / PAIRS_PER, *refs),
        out_shape=(
            jax.ShapeDtypeStruct((6, 6, PAIRS_PER), jnp.float32),
            jax.ShapeDtypeStruct((6, 1, 6), jnp.float32),
            jax.ShapeDtypeStruct((1, 6), jnp.float32),
        ),
        in_specs=[vmem],
        out_specs=(vmem, vmem, vmem),
        name="finish",
    )(shares)
    return jnp.transpose(cross, (2, 0, 1)), jnp.transpose(hessian, (1, 0, 2)), gradient


def solution(mesh):
    in_specs = (
        P("pair", "split", None),
        P("pair", None, "split"),
        P("pair", None, "split"),
        P(),
        P("pair"),
        P(),
    )
    out_specs = (P("pair", None, None), P("pair", None, None), P("pair", None))
    return jax.shard_map(
        per_device, mesh=mesh, in_specs=in_specs, out_specs=out_specs, check_vma=False
    )
```

```python
import math

import jax
import jax.numpy as jnp
from jax import lax
from jax.experimental import pallas as pl
from jax.experimental.pallas import tpu as pltpu
from jax.sharding import PartitionSpec as P


SIDE = 8
PAIRS_PER = 24
QUADS = SIDE // 2
SOURCES = 2 * SIDE
SLOTS = SOURCES * QUADS
ROWS = 128
WIDTH = 256
EXTRA = 8
PACKED = ROWS + EXTRA
LANES = 128
POSE = 42
HIGHEST = lax.Precision.HIGHEST

y_groups = [[z * SIDE + y for y in range(SIDE)] for z in range(SIDE)]
x_groups = [[2 * x + core for x in range(4)] for core in range(2)]
z_swap = [(z * SIDE + y, (z ^ 1) * SIDE + y) for z in range(SIDE) for y in range(SIDE)]
core_swap = [(s, s ^ 1) for s in range(8)]


def from_ahead(steps):
    return [(((z + steps) % SIDE) * SIDE + y, z * SIDE + y) for z in range(SIDE) for y in range(SIDE)]


def to_each(block, axis, groups):
    copies = jnp.broadcast_to(block, (len(groups[0]), *block.shape))
    return lax.all_to_all(copies, axis, split_axis=0, concat_axis=0, tiled=True, axis_index_groups=groups)


def nt(left, right, precision=None):
    return lax.dot_general(
        left, right, (((1,), (1,)), ((), ())), precision=precision, preferred_element_type=jnp.float32
    )


def cross_rows(u, v):
    return [
        u[1] * v[2] - u[2] * v[1],
        u[2] * v[0] - u[0] * v[2],
        u[0] * v[1] - u[1] * v[0],
    ]


def attend_kernel(scale, cnt_ref, base_ref, dst_ref, a1_ref, a2_ref, b1_ref, b2_ref, out_ref, a_ref, g_ref, h_ref, list_ref):
    a_ref[0:SIDE] = a1_ref[...]
    a_ref[SIDE:SOURCES] = a2_ref[...]
    for q in range(QUADS):
        for c, ref in enumerate((b1_ref, b2_ref)):
            for x in range(4):
                at = (c * 4 + x) * LANES
                g_ref[q, :, at : at + LANES] = ref[x, q, ROWS:PACKED, 0:LANES]
    h_ref[...] = jnp.zeros_like(h_ref)

    def scan(f, n):
        live = cnt_ref[f] > 0

        @pl.when(live)
        def _():
            list_ref[n] = f

        return n + live.astype(jnp.int32)

    n = lax.fori_loop(0, SLOTS, scan, jnp.int32(0))
    list_ref[n] = jnp.int32(SLOTS)
    row_ids = lax.broadcasted_iota(jnp.int32, (1, LANES), 1) + base_ref[0]

    def one(f):
        at = jnp.minimum(f, SLOTS - 1)
        q = at // SOURCES
        ia = at % SOURCES
        keys = jnp.concatenate(
            [ref[x, q, 0:ROWS, :] for ref in (b1_ref, b2_ref) for x in range(4)], axis=0
        )
        scores = nt(keys, a_ref[ia, 0:ROWS, :])
        top = jnp.max(scores, axis=0, keepdims=True)
        weights = jnp.exp2((scores - top) * scale)
        high = weights.astype(jnp.bfloat16)
        low = (weights - high.astype(jnp.float32)).astype(jnp.bfloat16)
        geometry = g_ref[q]
        moment = jnp.dot(geometry, high, preferred_element_type=jnp.float32) + jnp.dot(
            geometry, low, preferred_element_type=jnp.float32
        )
        softened = moment / moment[6:7]
        m = [softened[d : d + 1] for d in range(3)]
        v = [softened[3 + d : 4 + d] for d in range(3)]
        own = a_ref[ia, ROWS:PACKED, 0:LANES].astype(jnp.float32)
        s = [own[d : d + 1] for d in range(3)]
        residual = v[0] * (s[0] - m[0]) + v[1] * (s[1] - m[1]) + v[2] * (s[2] - m[2])
        zero = jnp.zeros_like(residual)
        jacobian = jnp.concatenate(
            cross_rows(s, v) + v + [-t for t in cross_rows(m, v)] + [-t for t in v] + [residual] + [zero] * 3,
            axis=0,
        )
        seen = (row_ids < cnt_ref[f]).astype(jnp.float32)
        h_ref[f] = nt(jacobian * seen, jacobian, HIGHEST)

    def two(t, carry):
        first = list_ref[2 * t]
        second = list_ref[2 * t + 1]
        one(first)
        one(second)
        return carry

    list_ref[n + 1] = jnp.int32(SLOTS)
    lax.fori_loop(0, (n + 1) // 2, two, 0)

    col = lax.broadcasted_iota(jnp.int32, (16, LANES), 0)
    lane = lax.broadcasted_iota(jnp.int32, (16, LANES), 1)
    flat_source = jnp.zeros((SLOTS, LANES), jnp.float32)
    flat_target = jnp.zeros((SLOTS, LANES), jnp.float32)
    flat_cross = jnp.zeros((SLOTS, LANES), jnp.float32)
    for r in range(6):
        tail = (col == 12) & (lane == 36 + r)
        pick_low = (((col < 6) & (lane == 6 * r + col)) | tail).astype(jnp.float32)
        in_high = (col >= 6) & (col < 12) & (lane == 6 * r + col - 6)
        pick_high = (in_high | tail).astype(jnp.float32)
        upper = h_ref[0:SLOTS, r, :]
        lower = h_ref[0:SLOTS, 6 + r, :]
        flat_source += jnp.dot(upper, pick_low, precision=HIGHEST, preferred_element_type=jnp.float32)
        flat_cross += jnp.dot(upper, in_high.astype(jnp.float32), precision=HIGHEST, preferred_element_type=jnp.float32)
        flat_target += jnp.dot(lower, pick_high, precision=HIGHEST, preferred_element_type=jnp.float32)
    dest = lax.broadcasted_iota(jnp.int32, (SIDE * SIDE, SLOTS), 0)
    to_source = (dest == dst_ref[0:1, :]).astype(jnp.float32)
    to_target = (dest == dst_ref[1:2, :]).astype(jnp.float32)
    to_owner = (dest == dst_ref[2:3, :]).astype(jnp.float32)
    pose = jnp.dot(to_source, flat_source, precision=HIGHEST, preferred_element_type=jnp.float32)
    pose += jnp.dot(to_target, flat_target, precision=HIGHEST, preferred_element_type=jnp.float32)
    owned = []
    for q in range(QUADS):
        here = slice(q * SOURCES, (q + 1) * SOURCES)
        moved = pltpu.roll(flat_cross[here], POSE + 36 * (q % 2), 1)
        owned.append(
            jnp.dot(to_owner[:, 0:SOURCES], moved, precision=HIGHEST, preferred_element_type=jnp.float32)
        )
    out_ref[:, 0, :] = pose + owned[0] + owned[1]
    out_ref[:, 1, :] = owned[2] + owned[3]


def collect_kernel(group_ref, quad_ref, got_ref, out_ref, even_ref, odd_ref):
    even_ref[...] = jnp.zeros_like(even_ref)
    odd_ref[...] = jnp.zeros_like(odd_ref)
    for t in range(PAIRS_PER):
        q = quad_ref[t]
        row = got_ref[group_ref[t], q // 2, :].reshape(1, LANES)
        side = (q % 2).astype(jnp.float32)
        even_ref[t : t + 1, :] = row * (1.0 - side)
        odd_ref[t : t + 1, :] = row * side
    even = pltpu.roll(even_ref[...], LANES - POSE, 1)
    odd = pltpu.roll(odd_ref[...], LANES - POSE - 36, 1)
    pose = jnp.sum(got_ref[:, 0, :], axis=0, keepdims=True)
    row_id = lax.broadcasted_iota(jnp.int32, (32, LANES), 0)
    both = jnp.where(row_id == PAIRS_PER, pose, even + odd)
    for s in range(8):
        out_ref[s] = both


def finish_kernel(task_scale, pose_scale, got_ref, cross_ref, hessian_ref, gradient_ref):
    total = got_ref[0]
    for s in range(1, 8):
        total += got_ref[s]
    pose = total[PAIRS_PER : PAIRS_PER + 1, :] * pose_scale
    padded = jnp.concatenate([total, jnp.zeros((LANES - 32, LANES), jnp.float32)], axis=0) * task_scale
    turned = padded.T
    for r in range(6):
        cross_ref[r] = turned[6 * r : 6 * r + 6, 0:PAIRS_PER]
        hessian_ref[r] = pose[:, 6 * r : 6 * r + 6]
    gradient_ref[...] = pose[:, 36:42]


def looked_up(table, ids):
    at = jnp.arange(table.shape[0], dtype=jnp.int32)
    return jnp.sum(jnp.where(at[None, :] == ids[:, None], table[None, :], 0), axis=1)


def per_device(descriptors, points, normals, pair_list, intersection, pose_index):
    own = lax.axis_index("pair")
    z, y = own // SIDE, own % SIDE
    parity = z % 2
    other = z + 1 - 2 * parity

    count_high = (intersection // 16).astype(jnp.bfloat16)
    count_low = (intersection % 16).astype(jnp.bfloat16)
    left = jnp.concatenate(
        [points[0], normals[0], jnp.ones((1, ROWS), jnp.bfloat16), jnp.zeros((1, ROWS), jnp.bfloat16)], axis=0
    )
    counts = jnp.pad(jnp.stack([count_high, count_low]), ((6, 0), (0, LANES - PAIRS_PER)))
    packed = jnp.concatenate([descriptors[0], jnp.concatenate([left, counts], axis=1)], axis=0)

    sources_row = to_each(packed, "pair", y_groups)
    targets_quad = jnp.stack([packed] + [lax.ppermute(packed, "pair", from_ahead(2 * q)) for q in range(1, QUADS)])
    targets_mine = to_each(targets_quad, "split", x_groups)
    sources_next = lax.ppermute(sources_row, "pair", z_swap)
    targets_peer = lax.ppermute(targets_mine, "split", core_swap)

    all_targets = pair_list[:, 1].reshape(SIDE, SIDE, PAIRS_PER)
    task_targets = jnp.concatenate(
        [lax.dynamic_slice_in_dim(all_targets, z, 1, 0)[0], lax.dynamic_slice_in_dim(all_targets, other, 1, 0)[0]], axis=0
    )
    quads = jnp.arange(QUADS, dtype=jnp.int32)
    target_ids = (z + 2 * quads) % SIDE * SIDE + y
    is_task = task_targets[None, :, :] == target_ids[:, None, None]
    next_counts = sources_next[:, ROWS + 6 :, LANES:]
    both = jnp.concatenate([sources_row[:, ROWS + 6 :, LANES:], next_counts], axis=0)
    both = both[:, :, :PAIRS_PER].astype(jnp.float32)
    seen_rows = (both[:, 0] * 16 + both[:, 1]).astype(jnp.int32)
    task_counts = jnp.sum(jnp.where(is_task, seen_rows[None], 0), axis=2).reshape(SLOTS)
    task_counts = jnp.pad(task_counts, (0, 64))

    slot = jnp.arange(SLOTS, dtype=jnp.int32)
    slot_source = slot % SOURCES
    source_ids = jnp.where(slot_source < SIDE, z * SIDE + slot_source, other * SIDE + slot_source - SIDE)
    slot_targets = (z + 2 * (slot // SOURCES)) % SIDE * SIDE + y
    destinations = jnp.stack(
        [looked_up(pose_index, source_ids), looked_up(pose_index, slot_targets), source_ids] + [slot] * 5
    )
    base = (lax.axis_index("split") * ROWS).reshape(1)

    smem = pl.BlockSpec(memory_space=pltpu.SMEM)
    vmem = pl.BlockSpec(memory_space=pltpu.VMEM)
    scale = WIDTH**-0.5 / math.log(2.0)
    send = pl.pallas_call(
        lambda *refs: attend_kernel(scale, *refs),
        out_shape=jax.ShapeDtypeStruct((SIDE * SIDE, 2, LANES), jnp.float32),
        in_specs=[smem, smem, vmem, vmem, vmem, vmem, vmem],
        out_specs=vmem,
        scratch_shapes=[
            pltpu.VMEM((SOURCES, PACKED, WIDTH), jnp.bfloat16),
            pltpu.VMEM((QUADS, EXTRA, 8 * LANES), jnp.bfloat16),
            pltpu.VMEM((SLOTS + 1, 16, 16), jnp.float32),
            pltpu.SMEM((SLOTS + 8,), jnp.int32),
        ],
        compiler_params=pltpu.CompilerParams(vmem_limit_bytes=48 * 1024 * 1024),
        name="attend",
    )(task_counts, base, destinations, sources_row, sources_next, targets_mine, targets_peer)
    got = lax.all_to_all(send, "pair", split_axis=0, concat_axis=0, tiled=True)

    my_targets = lax.dynamic_slice_in_dim(pair_list[:, 1], own * PAIRS_PER, PAIRS_PER, 0)
    target_z, target_y = my_targets // SIDE, my_targets % SIDE
    group_z = jnp.where(target_z % 2 == parity, z, other)
    group = group_z * SIDE + target_y
    quad = (target_z - group_z + SIDE) % SIDE // 2
    share = pl.pallas_call(
        collect_kernel,
        out_shape=jax.ShapeDtypeStruct((8, 32, LANES), jnp.float32),
        in_specs=[smem, smem, vmem],
        out_specs=vmem,
        scratch_shapes=[pltpu.VMEM((32, LANES), jnp.float32), pltpu.VMEM((32, LANES), jnp.float32)],
        name="collect",
    )(group, quad, got)
    shares = lax.all_to_all(share, "split", split_axis=0, concat_axis=0, tiled=True)

    task_scale = 1.0 / (ROWS * 8)
    cross, hessian, gradient = pl.pallas_call(
        lambda *refs: finish_kernel(task_scale, task_scale / PAIRS_PER, *refs),
        out_shape=(
            jax.ShapeDtypeStruct((6, 6, PAIRS_PER), jnp.float32),
            jax.ShapeDtypeStruct((6, 1, 6), jnp.float32),
            jax.ShapeDtypeStruct((1, 6), jnp.float32),
        ),
        in_specs=[vmem],
        out_specs=(vmem, vmem, vmem),
        name="finish",
    )(shares)
    return jnp.transpose(cross, (2, 0, 1)), jnp.transpose(hessian, (1, 0, 2)), gradient


def solution(mesh):
    in_specs = (
        P("pair", "split", None),
        P("pair", None, "split"),
        P("pair", None, "split"),
        P(),
        P("pair"),
        P(),
    )
    out_specs = (P("pair", None, None), P("pair", None, None), P("pair", None))
    return jax.shard_map(
        per_device, mesh=mesh, in_specs=in_specs, out_specs=out_specs, check_vma=False
    )
```

```python
import math

import jax
import jax.numpy as jnp
from jax import lax
from jax.experimental import pallas as pl
from jax.experimental.pallas import tpu as pltpu
from jax.sharding import PartitionSpec as P


SIDE = 8
PAIRS_PER = 24
QUADS = SIDE // 2
SOURCES = 2 * SIDE
SLOTS = SOURCES * QUADS
ROWS = 128
WIDTH = 256
EXTRA = 8
PACKED = ROWS + EXTRA
LANES = 128
POSE = 42
CHUNKS = 1
HIGHEST = lax.Precision.HIGHEST

y_groups = [[z * SIDE + y for y in range(SIDE)] for z in range(SIDE)]
x_groups = [[2 * x + core for x in range(4)] for core in range(2)]
z_swap = [(z * SIDE + y, (z ^ 1) * SIDE + y) for z in range(SIDE) for y in range(SIDE)]
core_swap = [(s, s ^ 1) for s in range(8)]


def from_ahead(steps):
    return [(((z + steps) % SIDE) * SIDE + y, z * SIDE + y) for z in range(SIDE) for y in range(SIDE)]


def to_each(block, axis, groups):
    copies = jnp.broadcast_to(block, (len(groups[0]), *block.shape))
    return lax.all_to_all(copies, axis, split_axis=0, concat_axis=0, tiled=True, axis_index_groups=groups)


def nt(left, right, precision=None):
    return lax.dot_general(
        left, right, (((1,), (1,)), ((), ())), precision=precision, preferred_element_type=jnp.float32
    )


def cross_rows(u, v):
    return [
        u[1] * v[2] - u[2] * v[1],
        u[2] * v[0] - u[0] * v[2],
        u[0] * v[1] - u[1] * v[0],
    ]


def attend_kernel(scale, cnt_ref, base_ref, dst_ref, a1_ref, a2_ref, b1_ref, b2_ref, out_ref, a_ref, g_ref, h_ref, list_ref, even_ref, odd_ref):
    a_ref[0:SIDE] = a1_ref[...]
    a_ref[SIDE:SOURCES] = a2_ref[...]
    for q in range(QUADS):
        for c, ref in enumerate((b1_ref, b2_ref)):
            for x in range(4):
                at = (c * 4 + x) * LANES
                g_ref[q, :, at : at + LANES] = ref[x, q, ROWS:PACKED, 0:LANES]
    h_ref[...] = jnp.zeros_like(h_ref)

    n = jnp.int32(0)
    for q in range(QUADS):

        def scan(ia, n, q=q):
            f = q * SOURCES + ia
            live = cnt_ref[f] > 0

            @pl.when(live)
            def _():
                list_ref[n] = f

            return n + live.astype(jnp.int32)

        n = lax.fori_loop(0, SOURCES, scan, n, unroll=True)
        list_ref[n] = jnp.int32(q * SOURCES + SLOTS)
        n += n % 2
    row_ids = lax.broadcasted_iota(jnp.int32, (1, LANES), 1) + base_ref[0]

    def block_of(entry, softened):
        f = entry % SLOTS
        ia = f % SOURCES
        count = jnp.where(entry < SLOTS, cnt_ref[f], 0)
        m = [softened[d : d + 1] for d in range(3)]
        v = [softened[3 + d : 4 + d] for d in range(3)]
        own = a_ref[ia, ROWS:PACKED, 0:LANES].astype(jnp.float32)
        s = [own[d : d + 1] for d in range(3)]
        residual = v[0] * (s[0] - m[0]) + v[1] * (s[1] - m[1]) + v[2] * (s[2] - m[2])
        zero = jnp.zeros_like(residual)
        jacobian = jnp.concatenate(
            cross_rows(s, v) + v + [-t for t in cross_rows(m, v)] + [-t for t in v] + [residual] + [zero] * 3,
            axis=0,
        )
        seen = (row_ids < count).astype(jnp.float32)
        h_ref[jnp.minimum(entry, SLOTS)] = nt(jacobian * seen, jacobian, HIGHEST)

    def score(pair, buffer):
        first = list_ref[2 * pair]
        second = list_ref[2 * pair + 1]
        q = (first % SLOTS) // SOURCES
        queries = jnp.concatenate(
            [a_ref[first % SOURCES, 0:ROWS, :], a_ref[second % SOURCES, 0:ROWS, :]], axis=0
        )
        tops = []
        for c, ref in enumerate((b1_ref, b2_ref)):
            keys = jnp.concatenate([ref[x, q, 0:ROWS, :] for x in range(4)], axis=0)
            part = nt(keys, queries)
            buffer[c * 4 * ROWS : (c + 1) * 4 * ROWS, :] = part
            tops.append(jnp.max(part, axis=0, keepdims=True))
        return jnp.maximum(tops[0], tops[1])

    def finish_pair(pair, buffer, top):
        first = list_ref[2 * pair]
        second = list_ref[2 * pair + 1]
        q = (first % SLOTS) // SOURCES
        moment = jnp.zeros((EXTRA, 2 * LANES), jnp.float32)
        for c in range(CHUNKS):
            here = slice(c * (8 * ROWS // CHUNKS), (c + 1) * (8 * ROWS // CHUNKS))
            weights = jnp.exp2((buffer[here, :] - top) * scale)
            high = weights.astype(jnp.bfloat16)
            low = (weights - high.astype(jnp.float32)).astype(jnp.bfloat16)
            geometry = g_ref[q, :, here]
            moment += jnp.dot(geometry, high, preferred_element_type=jnp.float32)
            moment += jnp.dot(geometry, low, preferred_element_type=jnp.float32)
        softened = moment / moment[6:7]
        block_of(first, softened[:, 0:LANES])
        block_of(second, softened[:, LANES:])

    pairs = n // 2
    for extra in range(4):
        list_ref[n + extra] = jnp.int32(SLOTS)

    def two(t, top):
        pair = 2 * t
        next_top = score(pair + 1, odd_ref)
        finish_pair(pair, even_ref, top)

        def go_on():
            after = score(pair + 2, even_ref)
            finish_pair(pair + 1, odd_ref, next_top)
            return after

        return lax.cond(pair + 1 < pairs, go_on, lambda: next_top)

    lax.fori_loop(0, (pairs + 1) // 2, two, score(0, even_ref))

    col = lax.broadcasted_iota(jnp.int32, (16, LANES), 0)
    lane = lax.broadcasted_iota(jnp.int32, (16, LANES), 1)
    flat_source = jnp.zeros((SLOTS, LANES), jnp.float32)
    flat_target = jnp.zeros((SLOTS, LANES), jnp.float32)
    flat_cross = jnp.zeros((SLOTS, LANES), jnp.float32)
    for r in range(6):
        tail = (col == 12) & (lane == 36 + r)
        pick_low = (((col < 6) & (lane == 6 * r + col)) | tail).astype(jnp.float32)
        in_high = (col >= 6) & (col < 12) & (lane == 6 * r + col - 6)
        pick_high = (in_high | tail).astype(jnp.float32)
        upper = h_ref[0:SLOTS, r, :]
        lower = h_ref[0:SLOTS, 6 + r, :]
        flat_source += jnp.dot(upper, pick_low, precision=HIGHEST, preferred_element_type=jnp.float32)
        flat_cross += jnp.dot(upper, in_high.astype(jnp.float32), precision=HIGHEST, preferred_element_type=jnp.float32)
        flat_target += jnp.dot(lower, pick_high, precision=HIGHEST, preferred_element_type=jnp.float32)
    dest = lax.broadcasted_iota(jnp.int32, (SIDE * SIDE, SLOTS), 0)
    to_source = (dest == dst_ref[0:1, :]).astype(jnp.float32)
    to_target = (dest == dst_ref[1:2, :]).astype(jnp.float32)
    to_owner = (dest == dst_ref[2:3, :]).astype(jnp.float32)
    pose = jnp.dot(to_source, flat_source, precision=HIGHEST, preferred_element_type=jnp.float32)
    pose += jnp.dot(to_target, flat_target, precision=HIGHEST, preferred_element_type=jnp.float32)
    owned = []
    for q in range(QUADS):
        here = slice(q * SOURCES, (q + 1) * SOURCES)
        moved = pltpu.roll(flat_cross[here], POSE + 36 * (q % 2), 1)
        owned.append(
            jnp.dot(to_owner[:, 0:SOURCES], moved, precision=HIGHEST, preferred_element_type=jnp.float32)
        )
    out_ref[:, 0, :] = pose + owned[0] + owned[1]
    out_ref[:, 1, :] = owned[2] + owned[3]


def collect_kernel(group_ref, quad_ref, got_ref, out_ref, even_ref, odd_ref):
    even_ref[...] = jnp.zeros_like(even_ref)
    odd_ref[...] = jnp.zeros_like(odd_ref)
    for t in range(PAIRS_PER):
        q = quad_ref[t]
        row = got_ref[group_ref[t], q // 2, :].reshape(1, LANES)
        side = (q % 2).astype(jnp.float32)
        even_ref[t : t + 1, :] = row * (1.0 - side)
        odd_ref[t : t + 1, :] = row * side
    even = pltpu.roll(even_ref[...], LANES - POSE, 1)
    odd = pltpu.roll(odd_ref[...], LANES - POSE - 36, 1)
    pose = jnp.sum(got_ref[:, 0, :], axis=0, keepdims=True)
    row_id = lax.broadcasted_iota(jnp.int32, (32, LANES), 0)
    both = jnp.where(row_id == PAIRS_PER, pose, even + odd)
    for s in range(8):
        out_ref[s] = both


def finish_kernel(task_scale, pose_scale, got_ref, cross_ref, hessian_ref, gradient_ref):
    total = got_ref[0]
    for s in range(1, 8):
        total += got_ref[s]
    pose = total[PAIRS_PER : PAIRS_PER + 1, :] * pose_scale
    padded = jnp.concatenate([total, jnp.zeros((LANES - 32, LANES), jnp.float32)], axis=0) * task_scale
    turned = padded.T
    for r in range(6):
        cross_ref[r] = turned[6 * r : 6 * r + 6, 0:PAIRS_PER]
        hessian_ref[r] = pose[:, 6 * r : 6 * r + 6]
    gradient_ref[...] = pose[:, 36:42]


def looked_up(table, ids):
    at = jnp.arange(table.shape[0], dtype=jnp.int32)
    return jnp.sum(jnp.where(at[None, :] == ids[:, None], table[None, :], 0), axis=1)


def attend_call(scale, *operands):
    smem = pl.BlockSpec(memory_space=pltpu.SMEM)
    vmem = pl.BlockSpec(memory_space=pltpu.VMEM)
    return pl.pallas_call(
        lambda *refs: attend_kernel(scale, *refs),
        out_shape=jax.ShapeDtypeStruct((SIDE * SIDE, 2, LANES), jnp.float32),
        in_specs=[smem, smem, vmem, vmem, vmem, vmem, vmem],
        out_specs=vmem,
        scratch_shapes=[
            pltpu.VMEM((SOURCES, PACKED, WIDTH), jnp.bfloat16),
            pltpu.VMEM((QUADS, EXTRA, 8 * LANES), jnp.bfloat16),
            pltpu.VMEM((SLOTS + 1, 16, 16), jnp.float32),
            pltpu.SMEM((SLOTS + 16,), jnp.int32),
            pltpu.VMEM((8 * ROWS, 2 * LANES), jnp.float32),
            pltpu.VMEM((8 * ROWS, 2 * LANES), jnp.float32),
        ],
        compiler_params=pltpu.CompilerParams(vmem_limit_bytes=48 * 1024 * 1024),
        name="attend",
    )(*operands)


def per_device(descriptors, points, normals, pair_list, intersection, pose_index):
    own = lax.axis_index("pair")
    z, y = own // SIDE, own % SIDE
    parity = z % 2
    other = z + 1 - 2 * parity

    count_high = (intersection // 16).astype(jnp.bfloat16)
    count_low = (intersection % 16).astype(jnp.bfloat16)
    left = jnp.concatenate(
        [points[0], normals[0], jnp.ones((1, ROWS), jnp.bfloat16), jnp.zeros((1, ROWS), jnp.bfloat16)], axis=0
    )
    counts = jnp.pad(jnp.stack([count_high, count_low]), ((6, 0), (0, LANES - PAIRS_PER)))
    packed = jnp.concatenate([descriptors[0], jnp.concatenate([left, counts], axis=1)], axis=0)

    sources_row = to_each(packed, "pair", y_groups)
    targets_quad = jnp.stack([packed] + [lax.ppermute(packed, "pair", from_ahead(2 * q)) for q in range(1, QUADS)])
    targets_mine = to_each(targets_quad, "split", x_groups)
    sources_next = lax.ppermute(sources_row, "pair", z_swap)
    targets_peer = lax.ppermute(targets_mine, "split", core_swap)

    all_targets = pair_list[:, 1].reshape(SIDE, SIDE, PAIRS_PER)
    task_targets = jnp.concatenate(
        [lax.dynamic_slice_in_dim(all_targets, z, 1, 0)[0], lax.dynamic_slice_in_dim(all_targets, other, 1, 0)[0]], axis=0
    )
    quads = jnp.arange(QUADS, dtype=jnp.int32)
    target_ids = (z + 2 * quads) % SIDE * SIDE + y
    is_task = task_targets[None, :, :] == target_ids[:, None, None]
    next_counts = sources_next[:, ROWS + 6 :, LANES:]
    both = jnp.concatenate([sources_row[:, ROWS + 6 :, LANES:], next_counts], axis=0)
    both = both[:, :, :PAIRS_PER].astype(jnp.float32)
    seen_rows = (both[:, 0] * 16 + both[:, 1]).astype(jnp.int32)
    task_counts = jnp.sum(jnp.where(is_task, seen_rows[None], 0), axis=2).reshape(SLOTS)
    task_counts = jnp.pad(task_counts, (0, 64))

    slot = jnp.arange(SLOTS, dtype=jnp.int32)
    slot_source = slot % SOURCES
    source_ids = jnp.where(slot_source < SIDE, z * SIDE + slot_source, other * SIDE + slot_source - SIDE)
    slot_targets = (z + 2 * (slot // SOURCES)) % SIDE * SIDE + y
    destinations = jnp.stack(
        [looked_up(pose_index, source_ids), looked_up(pose_index, slot_targets), source_ids] + [slot] * 5
    )
    base = (lax.axis_index("split") * ROWS).reshape(1)

    smem = pl.BlockSpec(memory_space=pltpu.SMEM)
    vmem = pl.BlockSpec(memory_space=pltpu.VMEM)
    scale = WIDTH**-0.5 / math.log(2.0)
    send = attend_call(scale, task_counts, base, destinations, sources_row, sources_next, targets_mine, targets_peer)
    got = lax.all_to_all(send, "pair", split_axis=0, concat_axis=0, tiled=True)

    my_targets = lax.dynamic_slice_in_dim(pair_list[:, 1], own * PAIRS_PER, PAIRS_PER, 0)
    target_z, target_y = my_targets // SIDE, my_targets % SIDE
    group_z = jnp.where(target_z % 2 == parity, z, other)
    group = group_z * SIDE + target_y
    quad = (target_z - group_z + SIDE) % SIDE // 2
    share = pl.pallas_call(
        collect_kernel,
        out_shape=jax.ShapeDtypeStruct((8, 32, LANES), jnp.float32),
        in_specs=[smem, smem, vmem],
        out_specs=vmem,
        scratch_shapes=[pltpu.VMEM((32, LANES), jnp.float32), pltpu.VMEM((32, LANES), jnp.float32)],
        name="collect",
    )(group, quad, got)
    shares = lax.all_to_all(share, "split", split_axis=0, concat_axis=0, tiled=True)

    task_scale = 1.0 / (ROWS * 8)
    cross, hessian, gradient = pl.pallas_call(
        lambda *refs: finish_kernel(task_scale, task_scale / PAIRS_PER, *refs),
        out_shape=(
            jax.ShapeDtypeStruct((6, 6, PAIRS_PER), jnp.float32),
            jax.ShapeDtypeStruct((6, 1, 6), jnp.float32),
            jax.ShapeDtypeStruct((1, 6), jnp.float32),
        ),
        in_specs=[vmem],
        out_specs=(vmem, vmem, vmem),
        name="finish",
    )(shares)
    return jnp.transpose(cross, (2, 0, 1)), jnp.transpose(hessian, (1, 0, 2)), gradient


def solution(mesh):
    in_specs = (
        P("pair", "split", None),
        P("pair", None, "split"),
        P("pair", None, "split"),
        P(),
        P("pair"),
        P(),
    )
    out_specs = (P("pair", None, None), P("pair", None, None), P("pair", None))
    return jax.shard_map(
        per_device, mesh=mesh, in_specs=in_specs, out_specs=out_specs, check_vma=False
    )
```

```python
import math

import jax
import jax.numpy as jnp
from jax import lax
from jax.experimental import pallas as pl
from jax.experimental.pallas import tpu as pltpu
from jax.sharding import PartitionSpec as P


SIDE = 8
PAIRS_PER = 24
QUADS = SIDE // 2
SOURCES = 2 * SIDE
SLOTS = SOURCES * QUADS
ROWS = 128
WIDTH = 256
EXTRA = 8
PACKED = ROWS + EXTRA
LANES = 128
POSE = 42
CHUNKS = 1
HIGHEST = lax.Precision.HIGHEST

y_groups = [[z * SIDE + y for y in range(SIDE)] for z in range(SIDE)]
z_swap = [(z * SIDE + y, (z ^ 1) * SIDE + y) for z in range(SIDE) for y in range(SIDE)]
core_swap = [(s, s ^ 1) for s in range(8)]


def from_ahead(steps):
    return [(((z + steps) % SIDE) * SIDE + y, z * SIDE + y) for z in range(SIDE) for y in range(SIDE)]


def x_ahead(steps):
    return [((x + steps) % 4 * 2 + core, x * 2 + core) for x in range(4) for core in range(2)]


def to_each(block, axis, groups):
    copies = jnp.broadcast_to(block, (len(groups[0]), *block.shape))
    return lax.all_to_all(copies, axis, split_axis=0, concat_axis=0, tiled=True, axis_index_groups=groups)


def nt(left, right, precision=None):
    return lax.dot_general(
        left, right, (((1,), (1,)), ((), ())), precision=precision, preferred_element_type=jnp.float32
    )


def cross_rows(u, v):
    return [
        u[1] * v[2] - u[2] * v[1],
        u[2] * v[0] - u[0] * v[2],
        u[0] * v[1] - u[1] * v[0],
    ]


def attend_kernel(scale, cnt_ref, base_ref, dst_ref, a1_ref, a2_ref, *rest):
    b_refs, (out_ref, a_ref, g_ref, h_ref, list_ref, even_ref, odd_ref) = rest[:8], rest[8:]
    a_ref[0:SIDE] = a1_ref[...]
    a_ref[SIDE:SOURCES] = a2_ref[...]
    for q in range(QUADS):
        for x, ref in enumerate(b_refs):
            g_ref[q, :, x * LANES : (x + 1) * LANES] = ref[q, ROWS:PACKED, 0:LANES]
    h_ref[...] = jnp.zeros_like(h_ref)

    n = jnp.int32(0)
    for q in range(QUADS):

        def scan(ia, n, q=q):
            f = q * SOURCES + ia
            live = cnt_ref[f] > 0

            @pl.when(live)
            def _():
                list_ref[n] = f

            return n + live.astype(jnp.int32)

        n = lax.fori_loop(0, SOURCES, scan, n, unroll=True)
        list_ref[n] = jnp.int32(q * SOURCES + SLOTS)
        n += n % 2
    row_ids = lax.broadcasted_iota(jnp.int32, (1, LANES), 1) + base_ref[0]

    def block_of(entry, softened):
        f = entry % SLOTS
        ia = f % SOURCES
        count = jnp.where(entry < SLOTS, cnt_ref[f], 0)
        m = [softened[d : d + 1] for d in range(3)]
        v = [softened[3 + d : 4 + d] for d in range(3)]
        own = a_ref[ia, ROWS:PACKED, 0:LANES].astype(jnp.float32)
        s = [own[d : d + 1] for d in range(3)]
        residual = v[0] * (s[0] - m[0]) + v[1] * (s[1] - m[1]) + v[2] * (s[2] - m[2])
        zero = jnp.zeros_like(residual)
        jacobian = jnp.concatenate(
            cross_rows(s, v) + v + [-t for t in cross_rows(m, v)] + [-t for t in v] + [residual] + [zero] * 3,
            axis=0,
        )
        seen = (row_ids < count).astype(jnp.float32)
        h_ref[jnp.minimum(entry, SLOTS)] = nt(jacobian * seen, jacobian, HIGHEST)

    def score(pair, buffer):
        first = list_ref[2 * pair]
        second = list_ref[2 * pair + 1]
        q = (first % SLOTS) // SOURCES
        queries = jnp.concatenate(
            [a_ref[first % SOURCES, 0:ROWS, :], a_ref[second % SOURCES, 0:ROWS, :]], axis=0
        )
        tops = []
        for c in range(2):
            keys = jnp.concatenate([ref[q, 0:ROWS, :] for ref in b_refs[4 * c : 4 * c + 4]], axis=0)
            part = nt(keys, queries)
            buffer[c * 4 * ROWS : (c + 1) * 4 * ROWS, :] = part
            tops.append(jnp.max(part, axis=0, keepdims=True))
        return jnp.maximum(tops[0], tops[1])

    def finish_pair(pair, buffer, top):
        first = list_ref[2 * pair]
        second = list_ref[2 * pair + 1]
        q = (first % SLOTS) // SOURCES
        moment = jnp.zeros((EXTRA, 2 * LANES), jnp.float32)
        for c in range(CHUNKS):
            here = slice(c * (8 * ROWS // CHUNKS), (c + 1) * (8 * ROWS // CHUNKS))
            weights = jnp.exp2((buffer[here, :] - top) * scale)
            high = weights.astype(jnp.bfloat16)
            low = (weights - high.astype(jnp.float32)).astype(jnp.bfloat16)
            geometry = g_ref[q, :, here]
            moment += jnp.dot(geometry, high, preferred_element_type=jnp.float32)
            moment += jnp.dot(geometry, low, preferred_element_type=jnp.float32)
        softened = moment / moment[6:7]
        block_of(first, softened[:, 0:LANES])
        block_of(second, softened[:, LANES:])

    pairs = n // 2
    for extra in range(4):
        list_ref[n + extra] = jnp.int32(SLOTS)

    def two(t, top):
        pair = 2 * t
        next_top = score(pair + 1, odd_ref)
        finish_pair(pair, even_ref, top)

        def go_on():
            after = score(pair + 2, even_ref)
            finish_pair(pair + 1, odd_ref, next_top)
            return after

        return lax.cond(pair + 1 < pairs, go_on, lambda: next_top)

    lax.fori_loop(0, (pairs + 1) // 2, two, score(0, even_ref))

    col = lax.broadcasted_iota(jnp.int32, (16, LANES), 0)
    lane = lax.broadcasted_iota(jnp.int32, (16, LANES), 1)
    flat_source = jnp.zeros((SLOTS, LANES), jnp.float32)
    flat_target = jnp.zeros((SLOTS, LANES), jnp.float32)
    flat_cross = jnp.zeros((SLOTS, LANES), jnp.float32)
    for r in range(6):
        tail = (col == 12) & (lane == 36 + r)
        pick_low = (((col < 6) & (lane == 6 * r + col)) | tail).astype(jnp.float32)
        in_high = (col >= 6) & (col < 12) & (lane == 6 * r + col - 6)
        pick_high = (in_high | tail).astype(jnp.float32)
        upper = h_ref[0:SLOTS, r, :]
        lower = h_ref[0:SLOTS, 6 + r, :]
        flat_source += jnp.dot(upper, pick_low, precision=HIGHEST, preferred_element_type=jnp.float32)
        flat_cross += jnp.dot(upper, in_high.astype(jnp.float32), precision=HIGHEST, preferred_element_type=jnp.float32)
        flat_target += jnp.dot(lower, pick_high, precision=HIGHEST, preferred_element_type=jnp.float32)
    dest = lax.broadcasted_iota(jnp.int32, (SIDE * SIDE, SLOTS), 0)
    to_source = (dest == dst_ref[0:1, :]).astype(jnp.float32)
    to_target = (dest == dst_ref[1:2, :]).astype(jnp.float32)
    to_owner = (dest == dst_ref[2:3, :]).astype(jnp.float32)
    pose = jnp.dot(to_source, flat_source, precision=HIGHEST, preferred_element_type=jnp.float32)
    pose += jnp.dot(to_target, flat_target, precision=HIGHEST, preferred_element_type=jnp.float32)
    owned = []
    for q in range(QUADS):
        here = slice(q * SOURCES, (q + 1) * SOURCES)
        moved = pltpu.roll(flat_cross[here], POSE + 36 * (q % 2), 1)
        owned.append(
            jnp.dot(to_owner[:, 0:SOURCES], moved, precision=HIGHEST, preferred_element_type=jnp.float32)
        )
    out_ref[:, 0, :] = pose + owned[0] + owned[1]
    out_ref[:, 1, :] = owned[2] + owned[3]


def collect_kernel(group_ref, quad_ref, got_ref, out_ref, even_ref, odd_ref):
    even_ref[...] = jnp.zeros_like(even_ref)
    odd_ref[...] = jnp.zeros_like(odd_ref)
    for t in range(PAIRS_PER):
        q = quad_ref[t]
        row = got_ref[group_ref[t], q // 2, :].reshape(1, LANES)
        side = (q % 2).astype(jnp.float32)
        even_ref[t : t + 1, :] = row * (1.0 - side)
        odd_ref[t : t + 1, :] = row * side
    even = pltpu.roll(even_ref[...], LANES - POSE, 1)
    odd = pltpu.roll(odd_ref[...], LANES - POSE - 36, 1)
    pose = jnp.sum(got_ref[:, 0, :], axis=0, keepdims=True)
    row_id = lax.broadcasted_iota(jnp.int32, (32, LANES), 0)
    both = jnp.where(row_id == PAIRS_PER, pose, even + odd)
    for s in range(8):
        out_ref[s] = both


def finish_kernel(task_scale, pose_scale, got_ref, cross_ref, hessian_ref, gradient_ref):
    total = got_ref[0]
    for s in range(1, 8):
        total += got_ref[s]
    pose = total[PAIRS_PER : PAIRS_PER + 1, :] * pose_scale
    padded = jnp.concatenate([total, jnp.zeros((LANES - 32, LANES), jnp.float32)], axis=0) * task_scale
    turned = padded.T
    for r in range(6):
        cross_ref[r] = turned[6 * r : 6 * r + 6, 0:PAIRS_PER]
        hessian_ref[r] = pose[:, 6 * r : 6 * r + 6]
    gradient_ref[...] = pose[:, 36:42]


def looked_up(table, ids):
    at = jnp.arange(table.shape[0], dtype=jnp.int32)
    return jnp.sum(jnp.where(at[None, :] == ids[:, None], table[None, :], 0), axis=1)


def attend_call(scale, *operands):
    smem = pl.BlockSpec(memory_space=pltpu.SMEM)
    vmem = pl.BlockSpec(memory_space=pltpu.VMEM)
    return pl.pallas_call(
        lambda *refs: attend_kernel(scale, *refs),
        out_shape=jax.ShapeDtypeStruct((SIDE * SIDE, 2, LANES), jnp.float32),
        in_specs=[smem, smem] + [vmem] * 11,
        out_specs=vmem,
        scratch_shapes=[
            pltpu.VMEM((SOURCES, PACKED, WIDTH), jnp.bfloat16),
            pltpu.VMEM((QUADS, EXTRA, 8 * LANES), jnp.bfloat16),
            pltpu.VMEM((SLOTS + 1, 16, 16), jnp.float32),
            pltpu.SMEM((SLOTS + 16,), jnp.int32),
            pltpu.VMEM((8 * ROWS, 2 * LANES), jnp.float32),
            pltpu.VMEM((8 * ROWS, 2 * LANES), jnp.float32),
        ],
        compiler_params=pltpu.CompilerParams(vmem_limit_bytes=48 * 1024 * 1024),
        name="attend",
    )(*operands)


def per_device(descriptors, points, normals, pair_list, intersection, pose_index):
    own = lax.axis_index("pair")
    z, y = own // SIDE, own % SIDE
    parity = z % 2
    other = z + 1 - 2 * parity

    count_high = (intersection // 16).astype(jnp.bfloat16)
    count_low = (intersection % 16).astype(jnp.bfloat16)
    left = jnp.concatenate(
        [points[0], normals[0], jnp.ones((1, ROWS), jnp.bfloat16), jnp.zeros((1, ROWS), jnp.bfloat16)], axis=0
    )
    counts = jnp.pad(jnp.stack([count_high, count_low]), ((6, 0), (0, LANES - PAIRS_PER)))
    packed = jnp.concatenate([descriptors[0], jnp.concatenate([left, counts], axis=1)], axis=0)

    sources_row = to_each(packed, "pair", y_groups)
    targets_quad = jnp.stack([packed] + [lax.ppermute(packed, "pair", from_ahead(2 * q)) for q in range(1, QUADS)])
    quarters, peers = [targets_quad], []
    for d in (1, 2, 3):
        quarters.append(lax.ppermute(targets_quad, "split", x_ahead(d)))
    sources_next = lax.ppermute(sources_row, "pair", z_swap)
    for d in range(4):
        peers.append(lax.ppermute(quarters[d], "split", core_swap))

    all_targets = pair_list[:, 1].reshape(SIDE, SIDE, PAIRS_PER)
    task_targets = jnp.concatenate(
        [lax.dynamic_slice_in_dim(all_targets, z, 1, 0)[0], lax.dynamic_slice_in_dim(all_targets, other, 1, 0)[0]], axis=0
    )
    quads = jnp.arange(QUADS, dtype=jnp.int32)
    target_ids = (z + 2 * quads) % SIDE * SIDE + y
    is_task = task_targets[None, :, :] == target_ids[:, None, None]
    both = jnp.concatenate([sources_row[:, ROWS + 6 :, LANES:], sources_next[:, ROWS + 6 :, LANES:]], axis=0)
    both = both[:, :, :PAIRS_PER].astype(jnp.float32)
    seen_rows = (both[:, 0] * 16 + both[:, 1]).astype(jnp.int32)
    task_counts = jnp.sum(jnp.where(is_task, seen_rows[None], 0), axis=2).reshape(SLOTS)
    task_counts = jnp.pad(task_counts, (0, 64))

    slot = jnp.arange(SLOTS, dtype=jnp.int32)
    slot_source = slot % SOURCES
    source_ids = jnp.where(slot_source < SIDE, z * SIDE + slot_source, other * SIDE + slot_source - SIDE)
    slot_targets = (z + 2 * (slot // SOURCES)) % SIDE * SIDE + y
    destinations = jnp.stack(
        [looked_up(pose_index, source_ids), looked_up(pose_index, slot_targets), source_ids] + [slot] * 5
    )
    base = (lax.axis_index("split") * ROWS).reshape(1)

    smem = pl.BlockSpec(memory_space=pltpu.SMEM)
    vmem = pl.BlockSpec(memory_space=pltpu.VMEM)
    scale = WIDTH**-0.5 / math.log(2.0)
    send = attend_call(scale, task_counts, base, destinations, sources_row, sources_next, *quarters, *peers)
    got = lax.all_to_all(send, "pair", split_axis=0, concat_axis=0, tiled=True)

    my_targets = lax.dynamic_slice_in_dim(pair_list[:, 1], own * PAIRS_PER, PAIRS_PER, 0)
    target_z, target_y = my_targets // SIDE, my_targets % SIDE
    group_z = jnp.where(target_z % 2 == parity, z, other)
    group = group_z * SIDE + target_y
    quad = (target_z - group_z + SIDE) % SIDE // 2
    share = pl.pallas_call(
        collect_kernel,
        out_shape=jax.ShapeDtypeStruct((8, 32, LANES), jnp.float32),
        in_specs=[smem, smem, vmem],
        out_specs=vmem,
        scratch_shapes=[pltpu.VMEM((32, LANES), jnp.float32), pltpu.VMEM((32, LANES), jnp.float32)],
        name="collect",
    )(group, quad, got)
    shares = lax.all_to_all(share, "split", split_axis=0, concat_axis=0, tiled=True)

    task_scale = 1.0 / (ROWS * 8)
    cross, hessian, gradient = pl.pallas_call(
        lambda *refs: finish_kernel(task_scale, task_scale / PAIRS_PER, *refs),
        out_shape=(
            jax.ShapeDtypeStruct((6, 6, PAIRS_PER), jnp.float32),
            jax.ShapeDtypeStruct((6, 1, 6), jnp.float32),
            jax.ShapeDtypeStruct((1, 6), jnp.float32),
        ),
        in_specs=[vmem],
        out_specs=(vmem, vmem, vmem),
        name="finish",
    )(shares)
    return jnp.transpose(cross, (2, 0, 1)), jnp.transpose(hessian, (1, 0, 2)), gradient


def solution(mesh):
    in_specs = (
        P("pair", "split", None),
        P("pair", None, "split"),
        P("pair", None, "split"),
        P(),
        P("pair"),
        P(),
    )
    out_specs = (P("pair", None, None), P("pair", None, None), P("pair", None))
    return jax.shard_map(
        per_device, mesh=mesh, in_specs=in_specs, out_specs=out_specs, check_vma=False
    )
```

```python
import math

import jax
import jax.numpy as jnp
from jax import lax
from jax.experimental import pallas as pl
from jax.experimental.pallas import tpu as pltpu
from jax.sharding import PartitionSpec as P


SIDE = 8
PAIRS_PER = 24
QUADS = SIDE // 2
SOURCES = 2 * SIDE
SLOTS = SOURCES * QUADS
ROWS = 128
WIDTH = 256
EXTRA = 8
PACKED = ROWS + EXTRA
LANES = 128
POSE = 42
CHUNKS = 1
HIGHEST = lax.Precision.HIGHEST

y_groups = [[z * SIDE + y for y in range(SIDE)] for z in range(SIDE)]
z_swap = [(z * SIDE + y, (z ^ 1) * SIDE + y) for z in range(SIDE) for y in range(SIDE)]
core_swap = [(s, s ^ 1) for s in range(8)]


def from_ahead(steps):
    return [(((z + steps) % SIDE) * SIDE + y, z * SIDE + y) for z in range(SIDE) for y in range(SIDE)]


def x_ahead(steps):
    return [((x + steps) % 4 * 2 + core, x * 2 + core) for x in range(4) for core in range(2)]


def nt(left, right, precision=None):
    return lax.dot_general(
        left, right, (((1,), (1,)), ((), ())), precision=precision, preferred_element_type=jnp.float32
    )


def cross_rows(u, v):
    return [
        u[1] * v[2] - u[2] * v[1],
        u[2] * v[0] - u[0] * v[2],
        u[0] * v[1] - u[1] * v[0],
    ]


def attend_kernel(scale, cnt_ref, base_ref, dst_ref, a1_ref, a2_ref, *rest):
    b_refs, (out_ref, a_ref, g_ref, h_ref, list_ref, even_ref, odd_ref) = rest[:8], rest[8:]
    a_ref[0:SIDE] = a1_ref[...]
    a_ref[SIDE:SOURCES] = a2_ref[...]
    for q in range(QUADS):
        for x, ref in enumerate(b_refs):
            g_ref[q, :, x * LANES : (x + 1) * LANES] = ref[q, ROWS:PACKED, 0:LANES]
    h_ref[...] = jnp.zeros_like(h_ref)

    n = jnp.int32(0)
    for q in range(QUADS):

        def scan(ia, n, q=q):
            f = q * SOURCES + ia
            live = cnt_ref[f] > 0

            @pl.when(live)
            def _():
                list_ref[n] = f

            return n + live.astype(jnp.int32)

        n = lax.fori_loop(0, SOURCES, scan, n, unroll=True)
        list_ref[n] = jnp.int32(q * SOURCES + SLOTS)
        n += n % 2
    row_ids = lax.broadcasted_iota(jnp.int32, (1, LANES), 1) + base_ref[0]

    def block_of(entry, softened):
        f = entry % SLOTS
        ia = f % SOURCES
        count = jnp.where(entry < SLOTS, cnt_ref[f], 0)
        m = [softened[d : d + 1] for d in range(3)]
        v = [softened[3 + d : 4 + d] for d in range(3)]
        own = a_ref[ia, ROWS:PACKED, 0:LANES].astype(jnp.float32)
        s = [own[d : d + 1] for d in range(3)]
        residual = v[0] * (s[0] - m[0]) + v[1] * (s[1] - m[1]) + v[2] * (s[2] - m[2])
        zero = jnp.zeros_like(residual)
        jacobian = jnp.concatenate(
            cross_rows(s, v) + v + [-t for t in cross_rows(m, v)] + [-t for t in v] + [residual] + [zero] * 3,
            axis=0,
        )
        seen = (row_ids < count).astype(jnp.float32)
        h_ref[jnp.minimum(entry, SLOTS)] = nt(jacobian * seen, jacobian, HIGHEST)

    def score(pair, buffer):
        first = list_ref[2 * pair]
        second = list_ref[2 * pair + 1]
        q = (first % SLOTS) // SOURCES
        queries = jnp.concatenate(
            [a_ref[first % SOURCES, 0:ROWS, :], a_ref[second % SOURCES, 0:ROWS, :]], axis=0
        )
        tops = []
        for c in range(2):
            keys = jnp.concatenate([ref[q, 0:ROWS, :] for ref in b_refs[4 * c : 4 * c + 4]], axis=0)
            part = nt(keys, queries)
            buffer[c * 4 * ROWS : (c + 1) * 4 * ROWS, :] = part
            tops.append(jnp.max(part, axis=0, keepdims=True))
        return jnp.maximum(tops[0], tops[1])

    def finish_pair(pair, buffer, top):
        first = list_ref[2 * pair]
        second = list_ref[2 * pair + 1]
        q = (first % SLOTS) // SOURCES
        moment = jnp.zeros((EXTRA, 2 * LANES), jnp.float32)
        for c in range(CHUNKS):
            here = slice(c * (8 * ROWS // CHUNKS), (c + 1) * (8 * ROWS // CHUNKS))
            weights = jnp.exp2((buffer[here, :] - top) * scale)
            high = weights.astype(jnp.bfloat16)
            low = (weights - high.astype(jnp.float32)).astype(jnp.bfloat16)
            geometry = g_ref[q, :, here]
            moment += jnp.dot(geometry, high, preferred_element_type=jnp.float32)
            moment += jnp.dot(geometry, low, preferred_element_type=jnp.float32)
        softened = moment / moment[6:7]
        block_of(first, softened[:, 0:LANES])
        block_of(second, softened[:, LANES:])

    pairs = n // 2
    for extra in range(4):
        list_ref[n + extra] = jnp.int32(SLOTS)

    def two(t, top):
        pair = 2 * t
        next_top = score(pair + 1, odd_ref)
        finish_pair(pair, even_ref, top)

        def go_on():
            after = score(pair + 2, even_ref)
            finish_pair(pair + 1, odd_ref, next_top)
            return after

        return lax.cond(pair + 1 < pairs, go_on, lambda: next_top)

    lax.fori_loop(0, (pairs + 1) // 2, two, score(0, even_ref))

    col = lax.broadcasted_iota(jnp.int32, (16, LANES), 0)
    lane = lax.broadcasted_iota(jnp.int32, (16, LANES), 1)
    flat_source = jnp.zeros((SLOTS, LANES), jnp.float32)
    flat_target = jnp.zeros((SLOTS, LANES), jnp.float32)
    flat_cross = jnp.zeros((SLOTS, LANES), jnp.float32)
    for r in range(6):
        tail = (col == 12) & (lane == 36 + r)
        pick_low = (((col < 6) & (lane == 6 * r + col)) | tail).astype(jnp.float32)
        in_high = (col >= 6) & (col < 12) & (lane == 6 * r + col - 6)
        pick_high = (in_high | tail).astype(jnp.float32)
        upper = h_ref[0:SLOTS, r, :]
        lower = h_ref[0:SLOTS, 6 + r, :]
        flat_source += jnp.dot(upper, pick_low, precision=HIGHEST, preferred_element_type=jnp.float32)
        flat_cross += jnp.dot(upper, in_high.astype(jnp.float32), precision=HIGHEST, preferred_element_type=jnp.float32)
        flat_target += jnp.dot(lower, pick_high, precision=HIGHEST, preferred_element_type=jnp.float32)
    dest = lax.broadcasted_iota(jnp.int32, (SIDE * SIDE, SLOTS), 0)
    to_source = (dest == dst_ref[0:1, :]).astype(jnp.float32)
    to_target = (dest == dst_ref[1:2, :]).astype(jnp.float32)
    to_owner = (dest == dst_ref[2:3, :]).astype(jnp.float32)
    pose = jnp.dot(to_source, flat_source, precision=HIGHEST, preferred_element_type=jnp.float32)
    pose += jnp.dot(to_target, flat_target, precision=HIGHEST, preferred_element_type=jnp.float32)
    owned = []
    for q in range(QUADS):
        here = slice(q * SOURCES, (q + 1) * SOURCES)
        moved = pltpu.roll(flat_cross[here], POSE + 36 * (q % 2), 1)
        owned.append(
            jnp.dot(to_owner[:, 0:SOURCES], moved, precision=HIGHEST, preferred_element_type=jnp.float32)
        )
    out_ref[:, 0, :] = pose + owned[0] + owned[1]
    out_ref[:, 1, :] = owned[2] + owned[3]


def collect_kernel(group_ref, quad_ref, got_ref, out_ref, even_ref, odd_ref):
    even_ref[...] = jnp.zeros_like(even_ref)
    odd_ref[...] = jnp.zeros_like(odd_ref)
    for t in range(PAIRS_PER):
        q = quad_ref[t]
        row = got_ref[group_ref[t], q // 2, :].reshape(1, LANES)
        side = (q % 2).astype(jnp.float32)
        even_ref[t : t + 1, :] = row * (1.0 - side)
        odd_ref[t : t + 1, :] = row * side
    even = pltpu.roll(even_ref[...], LANES - POSE, 1)
    odd = pltpu.roll(odd_ref[...], LANES - POSE - 36, 1)
    pose = jnp.sum(got_ref[:, 0, :], axis=0, keepdims=True)
    row_id = lax.broadcasted_iota(jnp.int32, (32, LANES), 0)
    both = jnp.where(row_id == PAIRS_PER, pose, even + odd)
    for s in range(8):
        out_ref[s] = both


def finish_kernel(task_scale, pose_scale, got_ref, cross_ref, hessian_ref, gradient_ref):
    total = got_ref[0]
    for s in range(1, 8):
        total += got_ref[s]
    pose = total[PAIRS_PER : PAIRS_PER + 1, :] * pose_scale
    padded = jnp.concatenate([total, jnp.zeros((LANES - 32, LANES), jnp.float32)], axis=0) * task_scale
    turned = padded.T
    for r in range(6):
        cross_ref[r] = turned[6 * r : 6 * r + 6, 0:PAIRS_PER]
        hessian_ref[r] = pose[:, 6 * r : 6 * r + 6]
    gradient_ref[...] = pose[:, 36:42]


def looked_up(table, ids):
    at = jnp.arange(table.shape[0], dtype=jnp.int32)
    return jnp.sum(jnp.where(at[None, :] == ids[:, None], table[None, :], 0), axis=1)


def pack_kernel(desc_ref, points_ref, normals_ref, count_ref, packed_ref, copies_ref):
    count = count_ref[...]
    high = (count // 16).astype(jnp.float32)
    low = (count % 16).astype(jnp.float32)
    blank = jnp.zeros((1, LANES - PAIRS_PER), jnp.float32)
    right = jnp.concatenate(
        [
            jnp.zeros((6, LANES), jnp.float32),
            jnp.concatenate([high, blank], axis=1),
            jnp.concatenate([low, blank], axis=1),
        ],
        axis=0,
    )
    left = jnp.concatenate(
        [
            points_ref[...].astype(jnp.float32),
            normals_ref[...].astype(jnp.float32),
            jnp.ones((1, LANES), jnp.float32),
            jnp.zeros((1, LANES), jnp.float32),
        ],
        axis=0,
    )
    extra = jnp.concatenate([left, right], axis=1).astype(jnp.bfloat16)
    for ref in (packed_ref, *(copies_ref.at[i] for i in range(SIDE))):
        ref[0:ROWS, :] = desc_ref[...]
        ref[ROWS:PACKED, :] = extra


def pack_call(*operands):
    vmem = pl.BlockSpec(memory_space=pltpu.VMEM)
    return pl.pallas_call(
        pack_kernel,
        out_shape=(
            jax.ShapeDtypeStruct((PACKED, WIDTH), jnp.bfloat16),
            jax.ShapeDtypeStruct((SIDE, PACKED, WIDTH), jnp.bfloat16),
        ),
        in_specs=[vmem] * 4,
        out_specs=(vmem, vmem),
        name="pack",
    )(*operands)


def attend_call(scale, *operands):
    smem = pl.BlockSpec(memory_space=pltpu.SMEM)
    vmem = pl.BlockSpec(memory_space=pltpu.VMEM)
    return pl.pallas_call(
        lambda *refs: attend_kernel(scale, *refs),
        out_shape=jax.ShapeDtypeStruct((SIDE * SIDE, 2, LANES), jnp.float32),
        in_specs=[smem, smem] + [vmem] * 11,
        out_specs=vmem,
        scratch_shapes=[
            pltpu.VMEM((SOURCES, PACKED, WIDTH), jnp.bfloat16),
            pltpu.VMEM((QUADS, EXTRA, 8 * LANES), jnp.bfloat16),
            pltpu.VMEM((SLOTS + 1, 16, 16), jnp.float32),
            pltpu.SMEM((SLOTS + 16,), jnp.int32),
            pltpu.VMEM((8 * ROWS, 2 * LANES), jnp.float32),
            pltpu.VMEM((8 * ROWS, 2 * LANES), jnp.float32),
        ],
        compiler_params=pltpu.CompilerParams(vmem_limit_bytes=48 * 1024 * 1024),
        name="attend",
    )(*operands)


def per_device(descriptors, points, normals, pair_list, intersection, pose_index):
    own = lax.axis_index("pair")
    z, y = own // SIDE, own % SIDE
    parity = z % 2
    other = z + 1 - 2 * parity

    packed, copies = pack_call(descriptors[0], points[0], normals[0], intersection.reshape(1, PAIRS_PER))

    sources_row = lax.all_to_all(copies, "pair", split_axis=0, concat_axis=0, tiled=True, axis_index_groups=y_groups)
    targets_quad = jnp.stack([packed] + [lax.ppermute(packed, "pair", from_ahead(2 * q)) for q in range(1, QUADS)])
    quarters, peers = [targets_quad], []
    for d in (1, 2, 3):
        quarters.append(lax.ppermute(targets_quad, "split", x_ahead(d)))
    sources_next = lax.ppermute(sources_row, "pair", z_swap)
    for d in range(4):
        peers.append(lax.ppermute(quarters[d], "split", core_swap))

    all_targets = pair_list[:, 1].reshape(SIDE, SIDE, PAIRS_PER)
    task_targets = jnp.concatenate(
        [lax.dynamic_slice_in_dim(all_targets, z, 1, 0)[0], lax.dynamic_slice_in_dim(all_targets, other, 1, 0)[0]], axis=0
    )
    quads = jnp.arange(QUADS, dtype=jnp.int32)
    target_ids = (z + 2 * quads) % SIDE * SIDE + y
    is_task = task_targets[None, :, :] == target_ids[:, None, None]
    both = jnp.concatenate([sources_row[:, ROWS + 6 :, LANES:], sources_next[:, ROWS + 6 :, LANES:]], axis=0)
    both = both[:, :, :PAIRS_PER].astype(jnp.float32)
    seen_rows = (both[:, 0] * 16 + both[:, 1]).astype(jnp.int32)
    task_counts = jnp.sum(jnp.where(is_task, seen_rows[None], 0), axis=2).reshape(SLOTS)
    task_counts = jnp.pad(task_counts, (0, 64))

    slot = jnp.arange(SLOTS, dtype=jnp.int32)
    slot_source = slot % SOURCES
    source_ids = jnp.where(slot_source < SIDE, z * SIDE + slot_source, other * SIDE + slot_source - SIDE)
    slot_targets = (z + 2 * (slot // SOURCES)) % SIDE * SIDE + y
    destinations = jnp.stack(
        [looked_up(pose_index, source_ids), looked_up(pose_index, slot_targets), source_ids] + [slot] * 5
    )
    base = (lax.axis_index("split") * ROWS).reshape(1)

    smem = pl.BlockSpec(memory_space=pltpu.SMEM)
    vmem = pl.BlockSpec(memory_space=pltpu.VMEM)
    scale = WIDTH**-0.5 / math.log(2.0)
    send = attend_call(scale, task_counts, base, destinations, sources_row, sources_next, *quarters, *peers)
    got = lax.all_to_all(send, "pair", split_axis=0, concat_axis=0, tiled=True)

    my_targets = lax.dynamic_slice_in_dim(pair_list[:, 1], own * PAIRS_PER, PAIRS_PER, 0)
    target_z, target_y = my_targets // SIDE, my_targets % SIDE
    group_z = jnp.where(target_z % 2 == parity, z, other)
    group = group_z * SIDE + target_y
    quad = (target_z - group_z + SIDE) % SIDE // 2
    share = pl.pallas_call(
        collect_kernel,
        out_shape=jax.ShapeDtypeStruct((8, 32, LANES), jnp.float32),
        in_specs=[smem, smem, vmem],
        out_specs=vmem,
        scratch_shapes=[pltpu.VMEM((32, LANES), jnp.float32), pltpu.VMEM((32, LANES), jnp.float32)],
        name="collect",
    )(group, quad, got)
    shares = lax.all_to_all(share, "split", split_axis=0, concat_axis=0, tiled=True)

    task_scale = 1.0 / (ROWS * 8)
    cross, hessian, gradient = pl.pallas_call(
        lambda *refs: finish_kernel(task_scale, task_scale / PAIRS_PER, *refs),
        out_shape=(
            jax.ShapeDtypeStruct((6, 6, PAIRS_PER), jnp.float32),
            jax.ShapeDtypeStruct((6, 1, 6), jnp.float32),
            jax.ShapeDtypeStruct((1, 6), jnp.float32),
        ),
        in_specs=[vmem],
        out_specs=(vmem, vmem, vmem),
        name="finish",
    )(shares)
    return jnp.transpose(cross, (2, 0, 1)), jnp.transpose(hessian, (1, 0, 2)), gradient


def solution(mesh):
    in_specs = (
        P("pair", "split", None),
        P("pair", None, "split"),
        P("pair", None, "split"),
        P(),
        P("pair"),
        P(),
    )
    out_specs = (P("pair", None, None), P("pair", None, None), P("pair", None))
    return jax.shard_map(
        per_device, mesh=mesh, in_specs=in_specs, out_specs=out_specs, check_vma=False
    )
```

```python
import math

import jax
import jax.numpy as jnp
from jax import lax
from jax.experimental import pallas as pl
from jax.experimental.pallas import tpu as pltpu
from jax.sharding import PartitionSpec as P


SIDE = 8
PAIRS_PER = 24
QUADS = SIDE // 2
SOURCES = 2 * SIDE
SLOTS = SOURCES * QUADS
ROWS = 128
WIDTH = 256
EXTRA = 8
PACKED = ROWS + EXTRA
LANES = 128
POSE = 42
CHUNKS = 1
HIGHEST = lax.Precision.HIGHEST

y_groups = [[z * SIDE + y for y in range(SIDE)] for z in range(SIDE)]
z_swap = [(z * SIDE + y, (z ^ 1) * SIDE + y) for z in range(SIDE) for y in range(SIDE)]
core_swap = [(s, s ^ 1) for s in range(8)]


def from_ahead(steps):
    return [(((z + steps) % SIDE) * SIDE + y, z * SIDE + y) for z in range(SIDE) for y in range(SIDE)]


def x_ahead(steps):
    return [((x + steps) % 4 * 2 + core, x * 2 + core) for x in range(4) for core in range(2)]


def nt(left, right, precision=None):
    return lax.dot_general(
        left, right, (((1,), (1,)), ((), ())), precision=precision, preferred_element_type=jnp.float32
    )


def cross_rows(u, v):
    return [
        u[1] * v[2] - u[2] * v[1],
        u[2] * v[0] - u[0] * v[2],
        u[0] * v[1] - u[1] * v[0],
    ]


def attend_kernel(scale, cnt_ref, base_ref, dst_ref, a1_ref, a2_ref, *rest):
    blocks, (out_ref, a_ref, g_ref, h_ref, list_ref, even_ref, odd_ref) = rest[:4], rest[4:]
    b_refs = [ref.at[i] for ref in blocks for i in range(ref.shape[0])]
    a_ref[0:SIDE] = a1_ref[...]
    a_ref[SIDE:SOURCES] = a2_ref[...]
    for q in range(QUADS):
        for x, ref in enumerate(b_refs):
            g_ref[q, :, x * LANES : (x + 1) * LANES] = ref[q, ROWS:PACKED, 0:LANES]
    h_ref[...] = jnp.zeros_like(h_ref)

    n = jnp.int32(0)
    for q in range(QUADS):

        def scan(ia, n, q=q):
            f = q * SOURCES + ia
            live = cnt_ref[f] > 0

            @pl.when(live)
            def _():
                list_ref[n] = f

            return n + live.astype(jnp.int32)

        n = lax.fori_loop(0, SOURCES, scan, n, unroll=True)
        list_ref[n] = jnp.int32(q * SOURCES + SLOTS)
        n += n % 2
    row_ids = lax.broadcasted_iota(jnp.int32, (1, LANES), 1) + base_ref[0]

    def block_of(entry, softened):
        f = entry % SLOTS
        ia = f % SOURCES
        count = jnp.where(entry < SLOTS, cnt_ref[f], 0)
        m = [softened[d : d + 1] for d in range(3)]
        v = [softened[3 + d : 4 + d] for d in range(3)]
        own = a_ref[ia, ROWS:PACKED, 0:LANES].astype(jnp.float32)
        s = [own[d : d + 1] for d in range(3)]
        residual = v[0] * (s[0] - m[0]) + v[1] * (s[1] - m[1]) + v[2] * (s[2] - m[2])
        zero = jnp.zeros_like(residual)
        jacobian = jnp.concatenate(
            cross_rows(s, v) + v + [-t for t in cross_rows(m, v)] + [-t for t in v] + [residual] + [zero] * 3,
            axis=0,
        )
        seen = (row_ids < count).astype(jnp.float32)
        h_ref[jnp.minimum(entry, SLOTS)] = nt(jacobian * seen, jacobian, HIGHEST)

    def score(pair, buffer):
        first = list_ref[2 * pair]
        second = list_ref[2 * pair + 1]
        q = (first % SLOTS) // SOURCES
        queries = jnp.concatenate(
            [a_ref[first % SOURCES, 0:ROWS, :], a_ref[second % SOURCES, 0:ROWS, :]], axis=0
        )
        tops = []
        for c in range(2):
            keys = jnp.concatenate([ref[q, 0:ROWS, :] for ref in b_refs[4 * c : 4 * c + 4]], axis=0)
            part = nt(keys, queries)
            buffer[c * 4 * ROWS : (c + 1) * 4 * ROWS, :] = part
            tops.append(jnp.max(part, axis=0, keepdims=True))
        return jnp.maximum(tops[0], tops[1])

    def finish_pair(pair, buffer, top):
        first = list_ref[2 * pair]
        second = list_ref[2 * pair + 1]
        q = (first % SLOTS) // SOURCES
        moment = jnp.zeros((EXTRA, 2 * LANES), jnp.float32)
        for c in range(CHUNKS):
            here = slice(c * (8 * ROWS // CHUNKS), (c + 1) * (8 * ROWS // CHUNKS))
            weights = jnp.exp2((buffer[here, :] - top) * scale)
            high = weights.astype(jnp.bfloat16)
            low = (weights - high.astype(jnp.float32)).astype(jnp.bfloat16)
            geometry = g_ref[q, :, here]
            moment += jnp.dot(geometry, high, preferred_element_type=jnp.float32)
            moment += jnp.dot(geometry, low, preferred_element_type=jnp.float32)
        softened = moment / moment[6:7]
        block_of(first, softened[:, 0:LANES])
        block_of(second, softened[:, LANES:])

    pairs = n // 2
    for extra in range(4):
        list_ref[n + extra] = jnp.int32(SLOTS)

    def two(t, top):
        pair = 2 * t
        next_top = score(pair + 1, odd_ref)
        finish_pair(pair, even_ref, top)

        def go_on():
            after = score(pair + 2, even_ref)
            finish_pair(pair + 1, odd_ref, next_top)
            return after

        return lax.cond(pair + 1 < pairs, go_on, lambda: next_top)

    lax.fori_loop(0, (pairs + 1) // 2, two, score(0, even_ref))

    col = lax.broadcasted_iota(jnp.int32, (16, LANES), 0)
    lane = lax.broadcasted_iota(jnp.int32, (16, LANES), 1)
    flat_both = jnp.zeros((SLOTS, 2 * LANES), jnp.float32)
    flat_target = jnp.zeros((SLOTS, LANES), jnp.float32)
    for r in range(6):
        tail = (col == 12) & (lane == 36 + r)
        pick_low = (((col < 6) & (lane == 6 * r + col)) | tail).astype(jnp.float32)
        in_high = (col >= 6) & (col < 12) & (lane == 6 * r + col - 6)
        pick_high = (in_high | tail).astype(jnp.float32)
        upper = h_ref[0:SLOTS, r, :]
        lower = h_ref[0:SLOTS, 6 + r, :]
        picks = jnp.concatenate([pick_low, in_high.astype(jnp.float32)], axis=1)
        flat_both += jnp.dot(upper, picks, precision=HIGHEST, preferred_element_type=jnp.float32)
        flat_target += jnp.dot(lower, pick_high, precision=HIGHEST, preferred_element_type=jnp.float32)
    dest = lax.broadcasted_iota(jnp.int32, (SIDE * SIDE, SLOTS), 0)
    to_source = (dest == dst_ref[0:1, :]).astype(jnp.float32)
    to_target = (dest == dst_ref[1:2, :]).astype(jnp.float32)
    to_owner = (dest == dst_ref[2:3, :]).astype(jnp.float32)
    flat_source, flat_cross = flat_both[:, 0:LANES], flat_both[:, LANES:]
    moved = [
        pltpu.roll(flat_cross[q * SOURCES : (q + 1) * SOURCES], POSE + 36 * (q % 2), 1) for q in range(QUADS)
    ]
    poses = jnp.concatenate([to_source, to_target], axis=1)
    flats = jnp.concatenate([flat_source, flat_target], axis=0)
    pose = jnp.dot(poses, flats, precision=HIGHEST, preferred_element_type=jnp.float32)
    owner = to_owner[:, 0 : 2 * SOURCES]
    owned = [
        jnp.dot(owner, jnp.concatenate(two, axis=0), precision=HIGHEST, preferred_element_type=jnp.float32)
        for two in (moved[:2], moved[2:])
    ]
    out_ref[:, 0, :] = pose + owned[0]
    out_ref[:, 1, :] = owned[1]


def collect_kernel(group_ref, quad_ref, got_ref, out_ref, even_ref, odd_ref):
    even_ref[...] = jnp.zeros_like(even_ref)
    odd_ref[...] = jnp.zeros_like(odd_ref)
    for t in range(PAIRS_PER):
        q = quad_ref[t]
        row = got_ref[group_ref[t], q // 2, :].reshape(1, LANES)
        side = (q % 2).astype(jnp.float32)
        even_ref[t : t + 1, :] = row * (1.0 - side)
        odd_ref[t : t + 1, :] = row * side
    even = pltpu.roll(even_ref[...], LANES - POSE, 1)
    odd = pltpu.roll(odd_ref[...], LANES - POSE - 36, 1)
    pose = jnp.sum(got_ref[:, 0, :], axis=0, keepdims=True)
    row_id = lax.broadcasted_iota(jnp.int32, (32, LANES), 0)
    both = jnp.where(row_id == PAIRS_PER, pose, even + odd)
    for s in range(8):
        out_ref[s] = both


def finish_kernel(task_scale, pose_scale, got_ref, cross_ref, hessian_ref, gradient_ref):
    total = got_ref[0]
    for s in range(1, 8):
        total += got_ref[s]
    pose = total[PAIRS_PER : PAIRS_PER + 1, :] * pose_scale
    padded = jnp.concatenate([total, jnp.zeros((LANES - 32, LANES), jnp.float32)], axis=0) * task_scale
    turned = padded.T
    for r in range(6):
        cross_ref[r] = turned[6 * r : 6 * r + 6, 0:PAIRS_PER]
        hessian_ref[r] = pose[:, 6 * r : 6 * r + 6]
    gradient_ref[...] = pose[:, 36:42]


def looked_up(table, ids):
    at = jnp.arange(table.shape[0], dtype=jnp.int32)
    return jnp.sum(jnp.where(at[None, :] == ids[:, None], table[None, :], 0), axis=1)


def pack_kernel(desc_ref, points_ref, normals_ref, count_ref, packed_ref, copies_ref):
    count = count_ref[...]
    high = (count // 16).astype(jnp.float32)
    low = (count % 16).astype(jnp.float32)
    blank = jnp.zeros((1, LANES - PAIRS_PER), jnp.float32)
    right = jnp.concatenate(
        [
            jnp.zeros((6, LANES), jnp.float32),
            jnp.concatenate([high, blank], axis=1),
            jnp.concatenate([low, blank], axis=1),
        ],
        axis=0,
    )
    left = jnp.concatenate(
        [
            points_ref[...].astype(jnp.float32),
            normals_ref[...].astype(jnp.float32),
            jnp.ones((1, LANES), jnp.float32),
            jnp.zeros((1, LANES), jnp.float32),
        ],
        axis=0,
    )
    extra = jnp.concatenate([left, right], axis=1).astype(jnp.bfloat16)
    for ref in (packed_ref, *(copies_ref.at[i] for i in range(SIDE))):
        ref[0:ROWS, :] = desc_ref[...]
        ref[ROWS:PACKED, :] = extra


def pack_call(*operands):
    vmem = pl.BlockSpec(memory_space=pltpu.VMEM)
    return pl.pallas_call(
        pack_kernel,
        out_shape=(
            jax.ShapeDtypeStruct((PACKED, WIDTH), jnp.bfloat16),
            jax.ShapeDtypeStruct((SIDE, PACKED, WIDTH), jnp.bfloat16),
        ),
        in_specs=[vmem] * 4,
        out_specs=(vmem, vmem),
        name="pack",
    )(*operands)


def attend_call(scale, *operands):
    smem = pl.BlockSpec(memory_space=pltpu.SMEM)
    vmem = pl.BlockSpec(memory_space=pltpu.VMEM)
    return pl.pallas_call(
        lambda *refs: attend_kernel(scale, *refs),
        out_shape=jax.ShapeDtypeStruct((SIDE * SIDE, 2, LANES), jnp.float32),
        in_specs=[smem, smem] + [vmem] * 7,
        out_specs=vmem,
        scratch_shapes=[
            pltpu.VMEM((SOURCES, PACKED, WIDTH), jnp.bfloat16),
            pltpu.VMEM((QUADS, EXTRA, 8 * LANES), jnp.bfloat16),
            pltpu.VMEM((SLOTS + 1, 16, 16), jnp.float32),
            pltpu.SMEM((SLOTS + 16,), jnp.int32),
            pltpu.VMEM((8 * ROWS, 2 * LANES), jnp.float32),
            pltpu.VMEM((8 * ROWS, 2 * LANES), jnp.float32),
        ],
        compiler_params=pltpu.CompilerParams(vmem_limit_bytes=48 * 1024 * 1024),
        name="attend",
    )(*operands)


def per_device(descriptors, points, normals, pair_list, intersection, pose_index):
    own = lax.axis_index("pair")
    z, y = own // SIDE, own % SIDE
    parity = z % 2
    other = z + 1 - 2 * parity

    packed, copies = pack_call(descriptors[0], points[0], normals[0], intersection.reshape(1, PAIRS_PER))

    sources_row = lax.all_to_all(copies, "pair", split_axis=0, concat_axis=0, tiled=True, axis_index_groups=y_groups)
    targets_quad = jnp.stack([packed] + [lax.ppermute(packed, "pair", from_ahead(2 * q)) for q in range(1, QUADS)])
    quarters, mine, peers = [targets_quad], [], []
    for d in (1, 2, 3):
        quarters.append(lax.ppermute(targets_quad, "split", x_ahead(d)))
    sources_next = lax.ppermute(sources_row, "pair", z_swap)
    mine.append(jnp.stack([quarters[d] for d in (0,)]))
    peers.append(lax.ppermute(mine[-1], "split", core_swap))
    mine.append(jnp.stack([quarters[d] for d in (1, 3, 2)]))
    peers.append(lax.ppermute(mine[-1], "split", core_swap))

    all_targets = pair_list[:, 1].reshape(SIDE, SIDE, PAIRS_PER)
    task_targets = jnp.concatenate(
        [lax.dynamic_slice_in_dim(all_targets, z, 1, 0)[0], lax.dynamic_slice_in_dim(all_targets, other, 1, 0)[0]], axis=0
    )
    quads = jnp.arange(QUADS, dtype=jnp.int32)
    target_ids = (z + 2 * quads) % SIDE * SIDE + y
    is_task = task_targets[None, :, :] == target_ids[:, None, None]
    both = jnp.concatenate([sources_row[:, ROWS + 6 :, LANES:], sources_next[:, ROWS + 6 :, LANES:]], axis=0)
    both = both[:, :, :PAIRS_PER].astype(jnp.float32)
    seen_rows = (both[:, 0] * 16 + both[:, 1]).astype(jnp.int32)
    task_counts = jnp.sum(jnp.where(is_task, seen_rows[None], 0), axis=2).reshape(SLOTS)
    task_counts = jnp.pad(task_counts, (0, 64))

    slot = jnp.arange(SLOTS, dtype=jnp.int32)
    slot_source = slot % SOURCES
    source_ids = jnp.where(slot_source < SIDE, z * SIDE + slot_source, other * SIDE + slot_source - SIDE)
    slot_targets = (z + 2 * (slot // SOURCES)) % SIDE * SIDE + y
    destinations = jnp.stack(
        [looked_up(pose_index, source_ids), looked_up(pose_index, slot_targets), source_ids] + [slot] * 5
    )
    base = (lax.axis_index("split") * ROWS).reshape(1)

    smem = pl.BlockSpec(memory_space=pltpu.SMEM)
    vmem = pl.BlockSpec(memory_space=pltpu.VMEM)
    scale = WIDTH**-0.5 / math.log(2.0)
    send = attend_call(scale, task_counts, base, destinations, sources_row, sources_next, *mine, *peers)
    got = lax.all_to_all(send, "pair", split_axis=0, concat_axis=0, tiled=True)

    my_targets = lax.dynamic_slice_in_dim(pair_list[:, 1], own * PAIRS_PER, PAIRS_PER, 0)
    target_z, target_y = my_targets // SIDE, my_targets % SIDE
    group_z = jnp.where(target_z % 2 == parity, z, other)
    group = group_z * SIDE + target_y
    quad = (target_z - group_z + SIDE) % SIDE // 2
    share = pl.pallas_call(
        collect_kernel,
        out_shape=jax.ShapeDtypeStruct((8, 32, LANES), jnp.float32),
        in_specs=[smem, smem, vmem],
        out_specs=vmem,
        scratch_shapes=[pltpu.VMEM((32, LANES), jnp.float32), pltpu.VMEM((32, LANES), jnp.float32)],
        name="collect",
    )(group, quad, got)
    shares = lax.all_to_all(share, "split", split_axis=0, concat_axis=0, tiled=True)

    task_scale = 1.0 / (ROWS * 8)
    cross, hessian, gradient = pl.pallas_call(
        lambda *refs: finish_kernel(task_scale, task_scale / PAIRS_PER, *refs),
        out_shape=(
            jax.ShapeDtypeStruct((6, 6, PAIRS_PER), jnp.float32),
            jax.ShapeDtypeStruct((6, 1, 6), jnp.float32),
            jax.ShapeDtypeStruct((1, 6), jnp.float32),
        ),
        in_specs=[vmem],
        out_specs=(vmem, vmem, vmem),
        name="finish",
    )(shares)
    return jnp.transpose(cross, (2, 0, 1)), jnp.transpose(hessian, (1, 0, 2)), gradient


def solution(mesh):
    in_specs = (
        P("pair", "split", None),
        P("pair", None, "split"),
        P("pair", None, "split"),
        P(),
        P("pair"),
        P(),
    )
    out_specs = (P("pair", None, None), P("pair", None, None), P("pair", None))
    return jax.shard_map(
        per_device, mesh=mesh, in_specs=in_specs, out_specs=out_specs, check_vma=False
    )
```

```python
import math

import jax
import jax.numpy as jnp
from jax import lax
from jax.experimental import pallas as pl
from jax.experimental.pallas import tpu as pltpu
from jax.sharding import PartitionSpec as P


SIDE = 8
PAIRS_PER = 24
QUADS = SIDE // 2
SOURCES = 2 * SIDE
SLOTS = SOURCES * QUADS
ROWS = 128
WIDTH = 256
EXTRA = 8
PACKED = ROWS + EXTRA
LANES = 128
POSE = 42
CHUNKS = 1
HIGHEST = lax.Precision.HIGHEST

y_groups = [[z * SIDE + y for y in range(SIDE)] for z in range(SIDE)]
z_swap = [(z * SIDE + y, (z ^ 1) * SIDE + y) for z in range(SIDE) for y in range(SIDE)]
core_swap = [(s, s ^ 1) for s in range(8)]


def from_ahead(steps):
    return [(((z + steps) % SIDE) * SIDE + y, z * SIDE + y) for z in range(SIDE) for y in range(SIDE)]


def x_ahead(steps):
    return [((x + steps) % 4 * 2 + core, x * 2 + core) for x in range(4) for core in range(2)]


def nt(left, right, precision=None):
    return lax.dot_general(
        left, right, (((1,), (1,)), ((), ())), precision=precision, preferred_element_type=jnp.float32
    )


def cross_rows(u, v):
    return [
        u[1] * v[2] - u[2] * v[1],
        u[2] * v[0] - u[0] * v[2],
        u[0] * v[1] - u[1] * v[0],
    ]


def attend_kernel(scale, cnt_ref, base_ref, dst_ref, a1_ref, a2_ref, *rest):
    blocks, (out_ref, a_ref, g_ref, h_ref, list_ref, even_ref, odd_ref) = rest[:4], rest[4:]
    b_refs = [ref.at[i] for ref in blocks for i in range(ref.shape[0])]
    a_ref[0:SIDE] = a1_ref[...]
    a_ref[SIDE:SOURCES] = a2_ref[...]
    for q in range(QUADS):
        for x, ref in enumerate(b_refs):
            g_ref[q, :, x * LANES : (x + 1) * LANES] = ref[q, ROWS:PACKED, 0:LANES]
    h_ref[...] = jnp.zeros_like(h_ref)

    n = jnp.int32(0)
    for q in range(QUADS):

        def scan(ia, n, q=q):
            f = q * SOURCES + ia
            live = cnt_ref[f] > 0

            @pl.when(live)
            def _():
                list_ref[n] = f

            return n + live.astype(jnp.int32)

        n = lax.fori_loop(0, SOURCES, scan, n, unroll=True)
        list_ref[n] = jnp.int32(q * SOURCES + SLOTS)
        n += n % 2
    row_ids = lax.broadcasted_iota(jnp.int32, (1, LANES), 1) + base_ref[0]

    def block_of(entry, softened):
        f = entry % SLOTS
        ia = f % SOURCES
        count = jnp.where(entry < SLOTS, cnt_ref[f], 0)
        m = [softened[d : d + 1] for d in range(3)]
        v = [softened[3 + d : 4 + d] for d in range(3)]
        own = a_ref[ia, ROWS:PACKED, 0:LANES].astype(jnp.float32)
        s = [own[d : d + 1] for d in range(3)]
        residual = v[0] * (s[0] - m[0]) + v[1] * (s[1] - m[1]) + v[2] * (s[2] - m[2])
        zero = jnp.zeros_like(residual)
        jacobian = jnp.concatenate(
            cross_rows(s, v) + v + [-t for t in cross_rows(m, v)] + [-t for t in v] + [residual] + [zero] * 3,
            axis=0,
        )
        seen = (row_ids < count).astype(jnp.float32)
        h_ref[jnp.minimum(entry, SLOTS)] = nt(jacobian * seen, jacobian, HIGHEST)

    def score(pair, buffer):
        first = list_ref[2 * pair]
        second = list_ref[2 * pair + 1]
        q = (first % SLOTS) // SOURCES
        queries = jnp.concatenate(
            [a_ref[first % SOURCES, 0:ROWS, :], a_ref[second % SOURCES, 0:ROWS, :]], axis=0
        )
        tops = []
        for c in range(2):
            keys = jnp.concatenate([ref[q, 0:ROWS, :] for ref in b_refs[4 * c : 4 * c + 4]], axis=0)
            part = nt(keys, queries)
            buffer[c * 4 * ROWS : (c + 1) * 4 * ROWS, :] = part
            tops.append(jnp.max(part, axis=0, keepdims=True))
        return jnp.maximum(tops[0], tops[1])

    def finish_pair(pair, buffer, top):
        first = list_ref[2 * pair]
        second = list_ref[2 * pair + 1]
        q = (first % SLOTS) // SOURCES
        moment = jnp.zeros((EXTRA, 2 * LANES), jnp.float32)
        for c in range(CHUNKS):
            here = slice(c * (8 * ROWS // CHUNKS), (c + 1) * (8 * ROWS // CHUNKS))
            weights = jnp.exp2((buffer[here, :] - top) * scale)
            high = weights.astype(jnp.bfloat16)
            low = (weights - high.astype(jnp.float32)).astype(jnp.bfloat16)
            geometry = g_ref[q, :, here]
            moment += jnp.dot(geometry, high, preferred_element_type=jnp.float32)
            moment += jnp.dot(geometry, low, preferred_element_type=jnp.float32)
        softened = moment / moment[6:7]
        block_of(first, softened[:, 0:LANES])
        block_of(second, softened[:, LANES:])

    pairs = n // 2
    for extra in range(4):
        list_ref[n + extra] = jnp.int32(SLOTS)

    def two(t, top):
        pair = 2 * t
        next_top = score(pair + 1, odd_ref)
        finish_pair(pair, even_ref, top)

        def go_on():
            after = score(pair + 2, even_ref)
            finish_pair(pair + 1, odd_ref, next_top)
            return after

        return lax.cond(pair + 1 < pairs, go_on, lambda: next_top)

    lax.fori_loop(0, (pairs + 1) // 2, two, score(0, even_ref))

    col = lax.broadcasted_iota(jnp.int32, (16, LANES), 0)
    lane = lax.broadcasted_iota(jnp.int32, (16, LANES), 1)
    flat = jnp.zeros((SLOTS, 3 * LANES), jnp.float32)
    for r in range(6):
        tail = (col == 12) & (lane == 36 + r)
        pick_low = (((col < 6) & (lane == 6 * r + col)) | tail).astype(jnp.float32)
        in_high = (col >= 6) & (col < 12) & (lane == 6 * r + col - 6)
        pick_high = (in_high | tail).astype(jnp.float32)
        upper = h_ref[0:SLOTS, r, :]
        lower = h_ref[0:SLOTS, 6 + r, :]
        none = jnp.zeros((16, LANES), jnp.float32)
        picks = jnp.concatenate(
            [
                jnp.concatenate([pick_low, in_high.astype(jnp.float32), none], axis=1),
                jnp.concatenate([none, none, pick_high], axis=1),
            ],
            axis=0,
        )
        both = jnp.concatenate([upper, lower], axis=1)
        flat += jnp.dot(both, picks, precision=HIGHEST, preferred_element_type=jnp.float32)
    dest = lax.broadcasted_iota(jnp.int32, (SIDE * SIDE, SLOTS), 0)
    to_source = (dest == dst_ref[0:1, :]).astype(jnp.float32)
    to_target = (dest == dst_ref[1:2, :]).astype(jnp.float32)
    to_owner = (dest == dst_ref[2:3, :]).astype(jnp.float32)
    flat_source, flat_cross, flat_target = (flat[:, i * LANES : (i + 1) * LANES] for i in range(3))
    moved = [
        pltpu.roll(flat_cross[q * SOURCES : (q + 1) * SOURCES], POSE + 36 * (q % 2), 1) for q in range(QUADS)
    ]
    poses = jnp.concatenate([to_source, to_target], axis=1)
    flats = jnp.concatenate([flat_source, flat_target], axis=0)
    pose = jnp.dot(poses, flats, precision=HIGHEST, preferred_element_type=jnp.float32)
    owner = to_owner[:, 0 : 2 * SOURCES]
    owned = [
        jnp.dot(owner, jnp.concatenate(two, axis=0), precision=HIGHEST, preferred_element_type=jnp.float32)
        for two in (moved[:2], moved[2:])
    ]
    out_ref[:, 0, :] = pose + owned[0]
    out_ref[:, 1, :] = owned[1]


def collect_kernel(group_ref, quad_ref, got_ref, out_ref, even_ref, odd_ref):
    even_ref[...] = jnp.zeros_like(even_ref)
    odd_ref[...] = jnp.zeros_like(odd_ref)
    for t in range(PAIRS_PER):
        q = quad_ref[t]
        row = got_ref[group_ref[t], q // 2, :].reshape(1, LANES)
        side = (q % 2).astype(jnp.float32)
        even_ref[t : t + 1, :] = row * (1.0 - side)
        odd_ref[t : t + 1, :] = row * side
    even = pltpu.roll(even_ref[...], LANES - POSE, 1)
    odd = pltpu.roll(odd_ref[...], LANES - POSE - 36, 1)
    pose = jnp.sum(got_ref[:, 0, :], axis=0, keepdims=True)
    row_id = lax.broadcasted_iota(jnp.int32, (32, LANES), 0)
    both = jnp.where(row_id == PAIRS_PER, pose, even + odd)
    for s in range(8):
        out_ref[s] = both


def finish_kernel(task_scale, pose_scale, got_ref, cross_ref, hessian_ref, gradient_ref):
    total = got_ref[0]
    for s in range(1, 8):
        total += got_ref[s]
    pose = total[PAIRS_PER : PAIRS_PER + 1, :] * pose_scale
    padded = jnp.concatenate([total, jnp.zeros((LANES - 32, LANES), jnp.float32)], axis=0) * task_scale
    turned = padded.T
    for r in range(6):
        cross_ref[r] = turned[6 * r : 6 * r + 6, 0:PAIRS_PER]
        hessian_ref[r] = pose[:, 6 * r : 6 * r + 6]
    gradient_ref[...] = pose[:, 36:42]


def looked_up(table, ids):
    at = jnp.arange(table.shape[0], dtype=jnp.int32)
    return jnp.sum(jnp.where(at[None, :] == ids[:, None], table[None, :], 0), axis=1)


def pack_kernel(desc_ref, points_ref, normals_ref, count_ref, packed_ref, copies_ref):
    count = count_ref[...]
    high = (count // 16).astype(jnp.float32)
    low = (count % 16).astype(jnp.float32)
    blank = jnp.zeros((1, LANES - PAIRS_PER), jnp.float32)
    right = jnp.concatenate(
        [
            jnp.zeros((6, LANES), jnp.float32),
            jnp.concatenate([high, blank], axis=1),
            jnp.concatenate([low, blank], axis=1),
        ],
        axis=0,
    )
    left = jnp.concatenate(
        [
            points_ref[...].astype(jnp.float32),
            normals_ref[...].astype(jnp.float32),
            jnp.ones((1, LANES), jnp.float32),
            jnp.zeros((1, LANES), jnp.float32),
        ],
        axis=0,
    )
    extra = jnp.concatenate([left, right], axis=1).astype(jnp.bfloat16)
    for ref in (packed_ref, *(copies_ref.at[i] for i in range(SIDE))):
        ref[0:ROWS, :] = desc_ref[...]
        ref[ROWS:PACKED, :] = extra


def pack_call(*operands):
    vmem = pl.BlockSpec(memory_space=pltpu.VMEM)
    return pl.pallas_call(
        pack_kernel,
        out_shape=(
            jax.ShapeDtypeStruct((PACKED, WIDTH), jnp.bfloat16),
            jax.ShapeDtypeStruct((SIDE, PACKED, WIDTH), jnp.bfloat16),
        ),
        in_specs=[vmem] * 4,
        out_specs=(vmem, vmem),
        name="pack",
    )(*operands)


def attend_call(scale, *operands):
    smem = pl.BlockSpec(memory_space=pltpu.SMEM)
    vmem = pl.BlockSpec(memory_space=pltpu.VMEM)
    return pl.pallas_call(
        lambda *refs: attend_kernel(scale, *refs),
        out_shape=jax.ShapeDtypeStruct((SIDE * SIDE, 2, LANES), jnp.float32),
        in_specs=[smem, smem] + [vmem] * 7,
        out_specs=vmem,
        scratch_shapes=[
            pltpu.VMEM((SOURCES, PACKED, WIDTH), jnp.bfloat16),
            pltpu.VMEM((QUADS, EXTRA, 8 * LANES), jnp.bfloat16),
            pltpu.VMEM((SLOTS + 1, 16, 16), jnp.float32),
            pltpu.SMEM((SLOTS + 16,), jnp.int32),
            pltpu.VMEM((8 * ROWS, 2 * LANES), jnp.float32),
            pltpu.VMEM((8 * ROWS, 2 * LANES), jnp.float32),
        ],
        compiler_params=pltpu.CompilerParams(vmem_limit_bytes=48 * 1024 * 1024),
        name="attend",
    )(*operands)


def per_device(descriptors, points, normals, pair_list, intersection, pose_index):
    own = lax.axis_index("pair")
    z, y = own // SIDE, own % SIDE
    parity = z % 2
    other = z + 1 - 2 * parity

    packed, copies = pack_call(descriptors[0], points[0], normals[0], intersection.reshape(1, PAIRS_PER))

    sources_row = lax.all_to_all(copies, "pair", split_axis=0, concat_axis=0, tiled=True, axis_index_groups=y_groups)
    targets_quad = jnp.stack([packed] + [lax.ppermute(packed, "pair", from_ahead(2 * q)) for q in range(1, QUADS)])
    quarters, mine, peers = [targets_quad], [], []
    for d in (1, 2, 3):
        quarters.append(lax.ppermute(targets_quad, "split", x_ahead(d)))
    sources_next = lax.ppermute(sources_row, "pair", z_swap)
    mine.append(jnp.stack([quarters[d] for d in (0,)]))
    peers.append(lax.ppermute(mine[-1], "split", core_swap))
    mine.append(jnp.stack([quarters[d] for d in (1, 3, 2)]))
    peers.append(lax.ppermute(mine[-1], "split", core_swap))

    all_targets = pair_list[:, 1].reshape(SIDE, SIDE, PAIRS_PER)
    task_targets = jnp.concatenate(
        [lax.dynamic_slice_in_dim(all_targets, z, 1, 0)[0], lax.dynamic_slice_in_dim(all_targets, other, 1, 0)[0]], axis=0
    )
    quads = jnp.arange(QUADS, dtype=jnp.int32)
    target_ids = (z + 2 * quads) % SIDE * SIDE + y
    is_task = task_targets[None, :, :] == target_ids[:, None, None]
    both = jnp.concatenate([sources_row[:, ROWS + 6 :, LANES:], sources_next[:, ROWS + 6 :, LANES:]], axis=0)
    both = both[:, :, :PAIRS_PER].astype(jnp.float32)
    seen_rows = (both[:, 0] * 16 + both[:, 1]).astype(jnp.int32)
    task_counts = jnp.sum(jnp.where(is_task, seen_rows[None], 0), axis=2).reshape(SLOTS)
    task_counts = jnp.pad(task_counts, (0, 64))

    slot = jnp.arange(SLOTS, dtype=jnp.int32)
    slot_source = slot % SOURCES
    source_ids = jnp.where(slot_source < SIDE, z * SIDE + slot_source, other * SIDE + slot_source - SIDE)
    slot_targets = (z + 2 * (slot // SOURCES)) % SIDE * SIDE + y
    destinations = jnp.stack(
        [looked_up(pose_index, source_ids), looked_up(pose_index, slot_targets), source_ids] + [slot] * 5
    )
    base = (lax.axis_index("split") * ROWS).reshape(1)

    smem = pl.BlockSpec(memory_space=pltpu.SMEM)
    vmem = pl.BlockSpec(memory_space=pltpu.VMEM)
    scale = WIDTH**-0.5 / math.log(2.0)
    send = attend_call(scale, task_counts, base, destinations, sources_row, sources_next, *mine, *peers)
    got = lax.all_to_all(send, "pair", split_axis=0, concat_axis=0, tiled=True)

    my_targets = lax.dynamic_slice_in_dim(pair_list[:, 1], own * PAIRS_PER, PAIRS_PER, 0)
    target_z, target_y = my_targets // SIDE, my_targets % SIDE
    group_z = jnp.where(target_z % 2 == parity, z, other)
    group = group_z * SIDE + target_y
    quad = (target_z - group_z + SIDE) % SIDE // 2
    share = pl.pallas_call(
        collect_kernel,
        out_shape=jax.ShapeDtypeStruct((8, 32, LANES), jnp.float32),
        in_specs=[smem, smem, vmem],
        out_specs=vmem,
        scratch_shapes=[pltpu.VMEM((32, LANES), jnp.float32), pltpu.VMEM((32, LANES), jnp.float32)],
        name="collect",
    )(group, quad, got)
    shares = lax.all_to_all(share, "split", split_axis=0, concat_axis=0, tiled=True)

    task_scale = 1.0 / (ROWS * 8)
    cross, hessian, gradient = pl.pallas_call(
        lambda *refs: finish_kernel(task_scale, task_scale / PAIRS_PER, *refs),
        out_shape=(
            jax.ShapeDtypeStruct((6, 6, PAIRS_PER), jnp.float32),
            jax.ShapeDtypeStruct((6, 1, 6), jnp.float32),
            jax.ShapeDtypeStruct((1, 6), jnp.float32),
        ),
        in_specs=[vmem],
        out_specs=(vmem, vmem, vmem),
        name="finish",
    )(shares)
    return jnp.transpose(cross, (2, 0, 1)), jnp.transpose(hessian, (1, 0, 2)), gradient


def solution(mesh):
    in_specs = (
        P("pair", "split", None),
        P("pair", None, "split"),
        P("pair", None, "split"),
        P(),
        P("pair"),
        P(),
    )
    out_specs = (P("pair", None, None), P("pair", None, None), P("pair", None))
    return jax.shard_map(
        per_device, mesh=mesh, in_specs=in_specs, out_specs=out_specs, check_vma=False
    )
```
